128 devices in a mesh: grp: 8 (over z, core), dev: 16 (over y, x).
Axes of the slice: x: 4, y: 4, z: 4, core: 2. Of those that a mesh axis runs over, the one named last changes fastest.
Arguments:
- points: float32 [3, 2097152], P(None, ('grp', 'dev')), may hold values from -6 to 6
- rhs: float32 [32, 2097152], P(None, ('grp', 'dev')), may hold values from -6 to 6
- leaf_count: int32 [8192], P(('grp', 'dev')), may hold values from 64 to 256
- near_list: int32 [8192, 8], P(('grp', 'dev')), may hold values from 0 to 8191, as said below
- leaf_basis: float32 [64, 2097152], P(None, ('grp', 'dev')), may hold values from -0.375 to 0.375
- leaf_transfer: float32 [64, 524288], P(None, ('grp', 'dev')), may hold values from -0.75 to 0.75
- leaf_parent: int32 [8192], P(('grp', 'dev')), may hold values from 0 to 1023, as said below
- nodes1: float32 [3, 65536], P(None, ('grp', 'dev')), may hold values from -6 to 6
- box_transfer: float32 [64, 65536], P(None, ('grp', 'dev')), may hold values from -0.75 to 0.75
- box_parent: int32 [1024], P(('grp', 'dev')), may hold values from 0 to 127, as said below
- far1: int32 [1024, 16], P(('grp', 'dev')), may hold values from 0 to 1023, as said below
- nodes2: float32 [3, 8192], replicated, may hold values from -6 to 6
- far2: int32 [128, 8], replicated, may hold values from 0 to 127, as said below
Outputs:
- result: float32 [32, 2097152], P(None, ('grp', 'dev'))
The draws below stay inside these ranges and needn't reach their ends.
Inputs may be any that keep to these rules, and one draw needn't show every extreme that they name: `near_list`: row c begins with c itself; its other 7 entries are distinct leaf blocks of the same group of 1024 blocks (c // 1024 alike), each different from c by at most 32. `leaf_parent`: leaf c's box lies on the same device: it is one of boxes (c // 64) * 8 to (c // 64 + 1) * 8 - 1, and every box has exactly 8 leaves. `box_parent`: box b's parent belongs to its group: it is one of (b // 128) * 16 to (b // 128 + 1) * 16 - 1, and every level-2 box has exactly 8 children. `far1`: row t names 16 distinct level-1 boxes of t's group (b // 128 alike), never t. `far2`: row t names 8 distinct level-2 boxes, never t.
All inputs are finite; a program needn't handle non-finite values.
Results may differ from the reference program's by a relative error of at most 0.00011.
Values sent between devices are 32-bit elements; how exact they have to be, the bound alone decides.
A program may use at most 128 MiB of HBM per device.

```python
import jax
import jax.numpy as jnp
from jax import lax

B = 256
K = 64
R = 32
LEAF_DEV = 64
NEAR = 8
CHILD = 8
FAR1 = 16
FAR2 = 8
REACH = 32
BOX1_DEV = 8
B2_GRP = 16
GLEAVES = 1024
G1 = 128
LEAVES = 8192
NPTS = 2097152
NB1 = 1024
NB2 = 128


def draw_near_list(key, part):
    key = jax.random.fold_in(key, 101)
    leaf = jnp.arange(LEAVES, dtype=jnp.int32)
    start = leaf // GLEAVES * GLEAVES
    offsets = jnp.concatenate([jnp.arange(-REACH, 0, dtype=jnp.int32), jnp.arange(1, REACH + 1, dtype=jnp.int32)])
    keys = jax.random.split(key, LEAVES)

    def single(sub, own, first):
        order = jax.random.permutation(sub, offsets)
        target = own + order
        outside = ((target < first) | (target >= first + GLEAVES)).astype(jnp.int32)
        pick = jnp.argsort(outside, stable=True)[:NEAR - 1]
        return jnp.concatenate([own[None], target[pick]]).astype(jnp.int32)
    return jax.vmap(single)(keys, leaf, start)


def draw_leaf_parent(key, part):
    key = jax.random.fold_in(key, 202)
    count = LEAVES // LEAF_DEV
    keys = jax.random.split(key, count)

    def single(sub, device):
        order = jax.random.permutation(sub, LEAF_DEV).astype(jnp.int32)
        return device * BOX1_DEV + order // CHILD
    return jax.vmap(single)(keys, jnp.arange(count, dtype=jnp.int32)).reshape(LEAVES).astype(jnp.int32)


def draw_box_parent(key, part):
    key = jax.random.fold_in(key, 303)
    count = NB1 // G1
    keys = jax.random.split(key, count)

    def single(sub, group):
        order = jax.random.permutation(sub, G1).astype(jnp.int32)
        return group * B2_GRP + order // CHILD
    return jax.vmap(single)(keys, jnp.arange(count, dtype=jnp.int32)).reshape(NB1).astype(jnp.int32)


def draw_far1(key, part):
    key = jax.random.fold_in(key, 404)
    boxes = jnp.arange(NB1, dtype=jnp.int32)
    keys = jax.random.split(key, NB1)
    steps_all = jnp.arange(1, G1, dtype=jnp.int32)

    def single(sub, box):
        order = jax.random.permutation(sub, steps_all)[:FAR1]
        first = box // G1 * G1
        return (first + (box - first + order) % G1).astype(jnp.int32)
    return jax.vmap(single)(keys, boxes)


def draw_far2(key, part):
    key = jax.random.fold_in(key, 505)
    boxes = jnp.arange(NB2, dtype=jnp.int32)
    keys = jax.random.split(key, NB2)
    steps_all = jnp.arange(1, NB2, dtype=jnp.int32)

    def single(sub, box):
        order = jax.random.permutation(sub, steps_all)[:FAR2]
        return ((box + order) % NB2).astype(jnp.int32)
    return jax.vmap(single)(keys, boxes)


def set_ends(values, own_key, smallest, largest):
    longest = values.shape.index(max(values.shape))
    spots = []
    for shift in (0, 1):
        where = [jax.random.randint(jax.random.fold_in(own_key, axis), (), 0, length) for axis, length in enumerate(values.shape)]
        where[longest] = (where[longest] + shift) % values.shape[longest]
        spots.append(tuple(where))
    return values.at[spots[0]].set(smallest).at[spots[1]].set(largest)


def steps_of(stream_key, dims, cuts, smallest, largest):
    def one(position, parts):
        steps = jax.random.uniform(jax.random.fold_in(jax.random.fold_in(stream_key, 6), position), (parts,), jnp.float32, smallest / len(cuts), largest / len(cuts))
        return jnp.repeat(jnp.exp(steps), dims[position] // parts).reshape((-1,) + (1,) * (len(dims) - position - 1))

    gain = one(*cuts[0])
    for cut in cuts[1:]:
        gain = gain * one(*cut)
    return gain


def noise(stream_key, dims, width, bound, cuts=(), held_as=jnp.bfloat16):
    gain = steps_of(stream_key, dims, cuts, -0.22, 0.18) if cuts else 1.0
    entries = jax.random.normal(stream_key, dims, jnp.float32) * width * gain
    return jnp.minimum(jnp.maximum(entries, -bound), bound).astype(held_as)


def setup_inputs(seed: int = 0) -> dict:
    arg_keys = jax.random.split(jax.random.key(seed), 14)
    points = noise(arg_keys[0], (3, NPTS), 1.0, 6.0, ((1, 128),), jnp.float32)
    rhs = noise(arg_keys[1], (R, NPTS), 1.0, 6.0, ((1, 128),), jnp.float32)
    leaf_count = set_ends(jax.random.randint(arg_keys[2], (LEAVES,), B // 4, B + 1), jax.random.fold_in(arg_keys[2], 1), B // 4, B).astype(jnp.int32)
    near_list = draw_near_list(jax.random.fold_in(arg_keys[13], 71), 0)
    leaf_basis = noise(arg_keys[4], (K, NPTS), B ** -0.5, 0.375, ((1, 128),), jnp.float32)
    leaf_transfer = noise(arg_keys[5], (K, LEAVES * K), K ** -0.5, 0.75, ((1, 128),), jnp.float32)
    leaf_parent = draw_leaf_parent(jax.random.fold_in(arg_keys[13], 71), 0)
    nodes1 = noise(arg_keys[7], (3, NB1 * K), 1.0, 6.0, ((1, 128),), jnp.float32)
    box_transfer = noise(arg_keys[8], (K, NB1 * K), K ** -0.5, 0.75, ((1, 128),), jnp.float32)
    box_parent = draw_box_parent(jax.random.fold_in(arg_keys[13], 71), 0)
    far1 = draw_far1(jax.random.fold_in(arg_keys[13], 71), 0)
    nodes2 = noise(arg_keys[11], (3, NB2 * K), 1.0, 6.0, (), jnp.float32)
    far2 = draw_far2(jax.random.fold_in(arg_keys[13], 71), 0)
    return {"points": points, "rhs": rhs, "leaf_count": leaf_count, "near_list": near_list, "leaf_basis": leaf_basis, "leaf_transfer": leaf_transfer, "leaf_parent": leaf_parent, "nodes1": nodes1, "box_transfer": box_transfer, "box_parent": box_parent, "far1": far1, "nodes2": nodes2, "far2": far2}


HIGH = lax.Precision.HIGHEST

def kernel(first, second):
    d_zero = first[0][:, None] - second[0][None, :]
    d_one = first[1][:, None] - second[1][None, :]
    d_two = first[2][:, None] - second[2][None, :]
    dist = d_zero * d_zero + d_one * d_one + d_two * d_two
    return lax.rsqrt(1.0 + 16.0 * dist)

def reference(points, rhs, leaf_count, near_list, leaf_basis, leaf_transfer, leaf_parent, nodes1, box_transfer, box_parent, far1, nodes2, far2):
    slots = jnp.arange(B, dtype=jnp.int32)
    mask = (slots[None, :] < leaf_count[:, None]).astype(jnp.float32)
    leaf_points = points.reshape(3, LEAVES, B).transpose(1, 0, 2)
    values = rhs.reshape(R, LEAVES, B).transpose(1, 0, 2) * mask[:, None, :]

    def near_leaf(own, index):
        source_points = leaf_points[index]
        source_values = values[index]
        tiles = jax.vmap(lambda src: kernel(src, own))(source_points)
        return jnp.einsum('nrj,nji->ri', source_values, tiles, precision=HIGH)

    def near_block(inputs):
        return jax.vmap(near_leaf)(inputs[0], inputs[1])
    blocks = LEAVES // LEAF_DEV
    near = lax.map(near_block, (leaf_points.reshape(blocks, LEAF_DEV, 3, B), near_list.reshape(blocks, LEAF_DEV, NEAR)))
    near = near.reshape(LEAVES, R, B)
    basis = leaf_basis.reshape(K, LEAVES, B).transpose(1, 0, 2)
    m_leaf = jnp.einsum('lkb,lrb->lkr', basis, values, precision=HIGH)
    e_mats = leaf_transfer.reshape(K, LEAVES, K).transpose(1, 0, 2)
    lifted = jnp.einsum('lij,lir->ljr', e_mats, m_leaf, precision=HIGH)
    m_one = jax.ops.segment_sum(lifted, leaf_parent, NB1)
    f_mats = box_transfer.reshape(K, NB1, K).transpose(1, 0, 2)
    raised = jnp.einsum('bij,bir->bjr', f_mats, m_one, precision=HIGH)
    m_two = jax.ops.segment_sum(raised, box_parent, NB2)
    node_one = nodes1.reshape(3, NB1, K).transpose(1, 0, 2)
    node_two = nodes2.reshape(3, NB2, K).transpose(1, 0, 2)

    def couple(target, sources, expansions):
        tiles = jax.vmap(lambda src: kernel(target, src))(sources)
        return jnp.einsum('sij,sjr->ir', tiles, expansions, precision=HIGH)
    l_one = jax.vmap(lambda t, idx: couple(t, node_one[idx], m_one[idx]))(node_one, far1)
    l_two = jax.vmap(lambda t, idx: couple(t, node_two[idx], m_two[idx]))(node_two, far2)
    g_one = l_one + jnp.einsum('bij,bjr->bir', f_mats, l_two[box_parent], precision=HIGH)
    g_leaf = jnp.einsum('lij,ljr->lir', e_mats, g_one[leaf_parent], precision=HIGH)
    far_part = jnp.einsum('lkr,lkb->lrb', g_leaf, basis, precision=HIGH)
    total = (near + far_part) * mask[:, None, :]
    return total.transpose(1, 0, 2).reshape(R, NPTS)
```

```python
import functools

import jax
import jax.numpy as jnp
from jax import lax
from jax.experimental import pallas as pl
from jax.experimental.pallas import tpu as pltpu
from jax.sharding import PartitionSpec as P

B = 256
K = 64
R = 32
NEAR = 8
CHILD = 8
REACH = 32


HIGH = lax.Precision.HIGHEST


def edges(cells, axis, width):
    dim = cells.ndim - 1
    count = lax.axis_size(axis)
    head = lax.slice_in_dim(cells, 0, width, axis=dim)
    tail = lax.slice_in_dim(cells, cells.shape[dim] - width, cells.shape[dim], axis=dim)
    return (
        lax.ppermute(tail, axis, [(i, i + 1) for i in range(count - 1)]),
        lax.ppermute(head, axis, [(i + 1, i) for i in range(count - 1)]),
    )


def copy_for_each(x, axis):
    devices = lax.axis_size(axis)
    return lax.all_to_all(jnp.broadcast_to(x[None], (devices, *x.shape)), axis, 0, 0, tiled=True)


def laid_out(parts, dim):
    parts = jnp.moveaxis(parts, 0, dim)
    lengths = parts.shape
    return parts.reshape(*lengths[:dim], lengths[dim] * lengths[dim + 1], *lengths[dim + 2 :])


def gathered_copies(x, axis, dim):
    parts = copy_for_each(x, axis)
    return laid_out(parts, dim)


def gathered_total(x, axis):
    parts = lax.all_gather(x, axis)
    return parts.sum(axis=0)


def kernel(first, second):
    d_zero = first[0][:, None] - second[0][None, :]
    d_one = first[1][:, None] - second[1][None, :]
    d_two = first[2][:, None] - second[2][None, :]
    dist = d_zero * d_zero + d_one * d_one + d_two * d_two
    return lax.rsqrt(1.0 + 16.0 * dist)


def couple(target, sources, expansions):
    tiles = jax.vmap(lambda src: kernel(target, src))(sources)
    return jnp.einsum("sij,sjr->ir", tiles, expansions, precision=HIGH)


LANES = 128
TILE = 32
SLOTS = 2
NEAR_VMEM = 60 * 1024 * 1024


def near_kernel(leaves, cnt, rel, left_x, left_p, own_x, own_p, right_x, right_p, far, out, xs, pb, ab, lists, turns, accs):
    halo = left_x.shape[1] // B
    total = leaves + 2 * halo
    lane = lax.broadcasted_iota(jnp.int32, (R, B), 1)

    def fill(src_x, src_p, first, count):
        def one(i, carry):
            at = pl.ds(pl.multiple_of(i * B, B), B)
            to = pl.ds(pl.multiple_of((first + i) * B, B), B)
            x = jnp.where(lane < cnt[first + i], src_x[:, at], 0.0)
            high = x.astype(jnp.bfloat16)
            xs[0:R, to] = high
            xs[R : 2 * R, to] = (x - high.astype(jnp.float32)).astype(jnp.bfloat16)
            pb[0:3, to] = src_p[:, at] * 4.0
            return carry

        lax.fori_loop(0, count, one, 0, unroll=4)

    fill(left_x, left_p, 0, halo)
    fill(own_x, own_p, halo, leaves)
    fill(right_x, right_p, halo + leaves, halo)
    tail = pl.ds(total * B, 2 * LANES)
    xs[:, tail] = jnp.zeros((2 * R, 2 * LANES), jnp.bfloat16)
    pb[:, tail] = jnp.zeros((8, 2 * LANES), jnp.float32)

    def prepare(slot, target):
        place = slot * 24
        for n in range(NEAR):
            src = rel[target * NEAR + n]
            lists[place] = 2 * src
            lists[place + 1] = 2 * src + 1
            place = place + 1 + (cnt[src] > LANES).astype(jnp.int32)
        for n in range(3):
            lists[place + n] = 2 * total
        turns[slot] = (place - slot * 24 + 1) // 2
        for half in range(B // LANES):
            at = pl.ds(pl.multiple_of((halo + target) * B + half * LANES, LANES), LANES)
            flipped = pb[:, at].T
            for d in range(3):
                ab[slot, d, half * LANES : (half + 1) * LANES, :] = jnp.broadcast_to(
                    flipped[:, d : d + 1], (LANES, LANES)
                )

    def finish(slot, target):
        parts = []
        for half in range(B // LANES):
            rows = []
            for t in range(half * LANES // TILE, (half + 1) * LANES // TILE):
                rows.append(
                    pltpu.matmul_pop(accs[0][slot][t])[:, :LANES] + pltpu.matmul_pop(accs[1][slot][t])[:, :LANES]
                )
            flipped = jnp.concatenate(rows, axis=0).T
            parts.append(flipped[0:R] + flipped[R : 2 * R])
        at = pl.ds(pl.multiple_of(target * B, B), B)
        value = jnp.concatenate(parts, axis=1) + far[:, at]
        out[:, at] = jnp.where(lane < cnt[halo + target], value, 0.0)

    def couple_chunk(slot, tiles, units, first):
        blocks = []
        for unit in units:
            cols, weights = [], []
            for half in range(2):
                at = lists[first + 2 * unit + half]
                at = pl.ds(pl.multiple_of(at * LANES, LANES), LANES)
                weights.append(xs[:, at])
                cols.append([pb[d : d + 1, at] for d in range(3)])
            w = jnp.concatenate(weights, axis=1)
            pltpu.matmul_push_rhs(jnp.concatenate([w] * 4, axis=0), 0, unit, transpose=True)
            blocks.append(cols)
        for t in range(tiles):
            rows = pl.ds(t * TILE, TILE)
            own = [ab[slot, d, rows, :] for d in range(3)]
            for unit in units:
                highs, lows = [], []
                for half in range(2):
                    col = blocks[unit][half]
                    d0, d1, d2 = (own[d] - col[d] for d in range(3))
                    k = lax.rsqrt(((1.0 + d0 * d0) + d1 * d1) + d2 * d2)
                    high = k.astype(jnp.bfloat16)
                    highs.append(high)
                    lows.append((k - high.astype(jnp.float32)).astype(jnp.bfloat16))
                acc = accs[unit][slot][t]
                pltpu.matmul_acc_lhs(acc, jnp.concatenate(highs, axis=1), load_staged_rhs=0 if t == 0 else None)
                pltpu.matmul_acc_lhs(acc, jnp.concatenate(lows, axis=1))

    def sweep(slot, tiles):
        count = turns[slot]

        def pair(i, carry):
            couple_chunk(slot, tiles, (0, 1), slot * 24 + 4 * i)
            return carry

        lax.fori_loop(0, count // 2, pair, 0)

        @pl.when(count % 2 == 1)
        def _():
            couple_chunk(slot, tiles, (0,), slot * 24 + 2 * (count - 1))

    def group(g, carry):
        for slot in range(SLOTS):
            finish(slot, jnp.maximum(g - 1, 0) * SLOTS + slot)
            prepare(slot, jnp.minimum(g, leaves // SLOTS - 1) * SLOTS + slot)

        @pl.when(g < leaves // SLOTS)
        def _():
            for slot in range(SLOTS):
                kind = (cnt[halo + g * SLOTS + slot] + TILE - 1) // TILE - 2
                lax.switch(kind, [functools.partial(sweep, slot, tiles) for tiles in range(2, B // TILE + 1)])

        return carry

    lax.fori_loop(0, leaves // SLOTS + 1, group, 0)


def near_body(leaves, *refs):
    tiles = B // TILE
    specs = tuple(
        tuple(tuple(pltpu.ACC(unit)((TILE, 256), jnp.float32) for _ in range(tiles)) for _ in range(SLOTS))
        for unit in range(2)
    )
    pl.run_scoped(lambda accs: near_kernel(leaves, *refs, accs), specs)


def near_field(cnt, rel, left_x, left_p, own_x, own_p, right_x, right_p, far):
    leaves = own_x.shape[1] // B
    wide = (leaves + 2 * (left_x.shape[1] // B)) * B + 2 * LANES
    vmem = pl.BlockSpec(memory_space=pltpu.VMEM)
    smem = pl.BlockSpec(memory_space=pltpu.SMEM)
    return pl.pallas_call(
        functools.partial(near_body, leaves),
        out_shape=jax.ShapeDtypeStruct((R, leaves * B), jnp.float32),
        in_specs=[smem, smem] + [vmem] * 7,
        out_specs=vmem,
        scratch_shapes=[
            pltpu.VMEM((2 * R, wide), jnp.bfloat16),
            pltpu.VMEM((8, wide), jnp.float32),
            pltpu.VMEM((SLOTS, 3, B, LANES), jnp.float32),
            pltpu.SMEM((SLOTS * 24,), jnp.int32),
            pltpu.SMEM((SLOTS,), jnp.int32),
        ],
        compiler_params=pltpu.CompilerParams(vmem_limit_bytes=NEAR_VMEM),
        cost_estimate=pl.CostEstimate(flops=10**9, bytes_accessed=10**7, transcendentals=10**7),
        name="near_field",
    )(cnt, rel, left_x, left_p, own_x, own_p, right_x, right_p, far)


def local(
    points,
    rhs,
    leaf_count,
    near_list,
    leaf_basis,
    leaf_transfer,
    leaf_parent,
    nodes1,
    box_transfer,
    box_parent,
    far1,
    nodes2,
    far2,
):
    leaves = leaf_count.shape[0]
    n_dev = lax.axis_size("dev")
    group = lax.axis_index("grp")
    device = group * n_dev + lax.axis_index("dev")
    first_leaf = device * leaves
    slots = jnp.arange(B, dtype=jnp.int32)
    mask = (slots[None, :] < leaf_count[:, None]).astype(jnp.float32)
    masked = (rhs.reshape(R, leaves, B) * mask[None, :, :]).reshape(R, leaves * B)
    stacked = jnp.concatenate([points, masked], axis=0)
    width = REACH
    left, right = edges(stacked, "dev", width * B)
    left_count, right_count = edges(leaf_count, "dev", width)
    counts = jnp.concatenate([left_count, leaf_count, right_count])
    relative = (near_list - first_leaf + width).reshape(-1)
    basis = leaf_basis.reshape(K, leaves, B)
    values = masked.reshape(R, leaves, B)
    m_leaf = jnp.einsum("klb,rlb->lkr", basis, values, precision=HIGH)
    e_mats = leaf_transfer.reshape(K, leaves, K)
    lifted = jnp.einsum("ilj,lir->ljr", e_mats, m_leaf, precision=HIGH)
    local_boxes = nodes1.shape[1] // K
    leaf_owner = leaf_parent - device * local_boxes
    leaf_onehot = (leaf_owner[:, None] == jnp.arange(local_boxes, dtype=jnp.int32)[None, :]).astype(
        jnp.float32
    )
    m_one = jnp.einsum("lb,ljr->bjr", leaf_onehot, lifted, precision=HIGH)
    group_boxes = local_boxes * n_dev
    coarse_group = group_boxes // CHILD
    coarse_base = group * coarse_group
    local_parent = box_parent - coarse_base
    parent_onehot = (
        local_parent[:, None] == jnp.arange(coarse_group, dtype=jnp.int32)[None, :]
    ).astype(jnp.float32)
    f_mats = box_transfer.reshape(K, local_boxes, K)
    group_m, group_nodes = (gathered_copies(m_one, "dev", 0), gathered_copies(nodes1, "dev", 1))
    raised = jnp.einsum("ibj,bir->bjr", f_mats, m_one, precision=HIGH)
    part = jnp.einsum("bp,bjr->pjr", parent_onehot, raised, precision=HIGH)
    m_two_group = gathered_total(part, "dev")
    node_group = group_nodes.reshape(3, group_boxes, K).transpose(1, 0, 2)
    own_nodes = nodes1.reshape(3, local_boxes, K).transpose(1, 0, 2)
    far_local = far1 - group * group_boxes
    l_one = jax.vmap(lambda t, idx: couple(t, node_group[idx], group_m[idx]))(own_nodes, far_local)
    m_two = gathered_copies(m_two_group, "grp", 0)
    total_coarse = nodes2.shape[1] // K
    node_two = nodes2.reshape(3, total_coarse, K).transpose(1, 0, 2)
    far_group = lax.dynamic_slice_in_dim(far2, coarse_base, coarse_group, 0)
    target_nodes = lax.dynamic_slice_in_dim(node_two, coarse_base, coarse_group, 0)
    l_two = jax.vmap(lambda t, idx: couple(t, node_two[idx], m_two[idx]))(target_nodes, far_group)
    chosen = jnp.einsum("bp,pjr->bjr", parent_onehot, l_two, precision=HIGH)
    g_one = l_one + jnp.einsum("ibj,bjr->bir", f_mats, chosen, precision=HIGH)
    picked = jnp.einsum("lb,bjr->ljr", leaf_onehot, g_one, precision=HIGH)
    g_leaf = jnp.einsum("ilj,ljr->lir", e_mats, picked, precision=HIGH)
    far_part = jnp.einsum("klb,lkr->lrb", basis, g_leaf, precision=HIGH)
    far_part = far_part.transpose(1, 0, 2).reshape(R, leaves * B)
    return near_field(counts, relative, left[3:], left[:3], rhs, points, right[3:], right[:3], far_part)


def solution(mesh):
    placed = (
        P(None, ("grp", "dev")),
        P(None, ("grp", "dev")),
        P(("grp", "dev")),
        P(("grp", "dev"), None),
        P(None, ("grp", "dev")),
        P(None, ("grp", "dev")),
        P(("grp", "dev")),
        P(None, ("grp", "dev")),
        P(None, ("grp", "dev")),
        P(("grp", "dev")),
        P(("grp", "dev"), None),
        P(),
        P(),
    )
    return jax.shard_map(
        local, mesh=mesh, in_specs=placed, out_specs=P(None, ("grp", "dev")), check_vma=False
    )
```

```python
import functools

import jax
import jax.numpy as jnp
from jax import lax
from jax.experimental import pallas as pl
from jax.experimental.pallas import tpu as pltpu
from jax.sharding import PartitionSpec as P

B = 256
K = 64
R = 32
NEAR = 8
REACH = 32
LANES = 128
TILE = 32
SLOTS = 2
NEAR_VMEM = 60 * 1024 * 1024


def near_kernel(leaves, place, halo_c, own_c, rel, halo_x, halo_p, own_x, own_p, far, out, xs, pb, ab, lists, cnt, turns, accs):
    halo = halo_x.shape[2] // B
    total = leaves + 2 * halo
    for i in range(halo):
        cnt[i] = halo_c[0, 0, leaves - halo + i]
        cnt[halo + leaves + i] = halo_c[2, 0, i]
    for i in range(leaves):
        cnt[halo + i] = own_c[i]
    lane = lax.broadcasted_iota(jnp.int32, (R, B), 1)

    def fill(src_x, src_p, first, count):
        def one(i, carry):
            at = pl.ds(pl.multiple_of(i * B, B), B)
            to = pl.ds(pl.multiple_of((first + i) * B, B), B)
            x = jnp.where(lane < cnt[first + i], src_x[:, at], 0.0)
            high = x.astype(jnp.bfloat16)
            xs[0:R, to] = high
            xs[R : 2 * R, to] = (x - high.astype(jnp.float32)).astype(jnp.bfloat16)
            pb[0:3, to] = src_p[:, at] * 4.0
            return carry

        lax.fori_loop(0, count, one, 0, unroll=4)

    fill(halo_x.at[0], halo_p.at[0], 0, halo)
    fill(own_x, own_p, halo, leaves)
    fill(halo_x.at[1], halo_p.at[1], halo + leaves, halo)
    tail = pl.ds(total * B, 2 * LANES)
    xs[:, tail] = jnp.zeros((2 * R, 2 * LANES), jnp.bfloat16)
    pb[:, tail] = jnp.zeros((8, 2 * LANES), jnp.float32)

    def prepare(slot, target):
        at = slot * 24
        for n in range(NEAR):
            src = rel[target, n] - place[1]
            lists[at] = 2 * src
            lists[at + 1] = 2 * src + 1
            at = at + 1 + (cnt[src] > LANES).astype(jnp.int32)
        for n in range(3):
            lists[at + n] = 2 * total
        turns[slot] = (at - slot * 24 + 1) // 2
        for half in range(B // LANES):
            at = pl.ds(pl.multiple_of((halo + target) * B + half * LANES, LANES), LANES)
            flipped = pb[:, at].T
            for d in range(3):
                ab[slot, d, half * LANES : (half + 1) * LANES, :] = jnp.broadcast_to(
                    flipped[:, d : d + 1], (LANES, LANES)
                )

    def finish(slot, target):
        parts = []
        for half in range(B // LANES):
            rows = []
            for t in range(half * LANES // TILE, (half + 1) * LANES // TILE):
                rows.append(
                    pltpu.matmul_pop(accs[0][slot][t])[:, :LANES] + pltpu.matmul_pop(accs[1][slot][t])[:, :LANES]
                )
            flipped = jnp.concatenate(rows, axis=0).T
            parts.append(flipped[0:R] + flipped[R : 2 * R])
        at = pl.ds(pl.multiple_of(target * B, B), B)
        value = jnp.concatenate(parts, axis=1) + far[:, at]
        out[:, at] = jnp.where(lane < cnt[halo + target], value, 0.0)

    def couple_chunk(slot, tiles, units, first):
        blocks = []
        for unit in units:
            cols, weights = [], []
            for half in range(2):
                at = lists[first + 2 * unit + half]
                at = pl.ds(pl.multiple_of(at * LANES, LANES), LANES)
                weights.append(xs[:, at])
                cols.append([pb[d : d + 1, at] for d in range(3)])
            w = jnp.concatenate(weights, axis=1)
            pltpu.matmul_push_rhs(jnp.concatenate([w] * 4, axis=0), 0, unit, transpose=True)
            blocks.append(cols)
        for t in range(tiles):
            rows = pl.ds(t * TILE, TILE)
            own = [ab[slot, d, rows, :] for d in range(3)]
            for unit in units:
                highs, lows = [], []
                for half in range(2):
                    col = blocks[unit][half]
                    d0, d1, d2 = (own[d] - col[d] for d in range(3))
                    k = lax.rsqrt(((1.0 + d0 * d0) + d1 * d1) + d2 * d2)
                    high = k.astype(jnp.bfloat16)
                    highs.append(high)
                    lows.append((k - high.astype(jnp.float32)).astype(jnp.bfloat16))
                acc = accs[unit][slot][t]
                pltpu.matmul_acc_lhs(acc, jnp.concatenate(highs, axis=1), load_staged_rhs=0 if t == 0 else None)
                pltpu.matmul_acc_lhs(acc, jnp.concatenate(lows, axis=1))

    def sweep(slot, tiles):
        count = turns[slot]

        def pair(i, carry):
            couple_chunk(slot, tiles, (0, 1), slot * 24 + 4 * i)
            return carry

        lax.fori_loop(0, count // 2, pair, 0)

        @pl.when(count % 2 == 1)
        def _():
            couple_chunk(slot, tiles, (0,), slot * 24 + 2 * (count - 1))

    def group(g, carry):
        for slot in range(SLOTS):
            finish(slot, jnp.maximum(g - 1, 0) * SLOTS + slot)
            prepare(slot, jnp.minimum(g, leaves // SLOTS - 1) * SLOTS + slot)

        @pl.when(g < leaves // SLOTS)
        def _():
            for slot in range(SLOTS):
                kind = (cnt[halo + g * SLOTS + slot] + TILE - 1) // TILE - 2
                lax.switch(kind, [functools.partial(sweep, slot, tiles) for tiles in range(2, B // TILE + 1)])

        return carry

    lax.fori_loop(0, leaves // SLOTS + 1, group, 0)


def near_body(leaves, *refs):
    tiles = B // TILE
    specs = tuple(
        tuple(tuple(pltpu.ACC(unit)((TILE, 256), jnp.float32) for _ in range(tiles)) for _ in range(SLOTS))
        for unit in range(2)
    )
    pl.run_scoped(lambda accs: near_kernel(leaves, *refs, accs), specs)


def near_field(place, halo_c, own_c, rel, halo_x, halo_p, own_x, own_p, far):
    leaves = own_x.shape[1] // B
    extent = leaves + 2 * (halo_x.shape[2] // B)
    wide = extent * B + 2 * LANES
    vmem = pl.BlockSpec(memory_space=pltpu.VMEM)
    smem = pl.BlockSpec(memory_space=pltpu.SMEM)
    return pl.pallas_call(
        functools.partial(near_body, leaves),
        out_shape=jax.ShapeDtypeStruct((R, leaves * B), jnp.float32),
        in_specs=[smem] * 4 + [vmem] * 5,
        out_specs=vmem,
        scratch_shapes=[
            pltpu.VMEM((2 * R, wide), jnp.bfloat16),
            pltpu.VMEM((8, wide), jnp.float32),
            pltpu.VMEM((SLOTS, 3, B, LANES), jnp.float32),
            pltpu.SMEM((SLOTS * 24,), jnp.int32),
            pltpu.SMEM((extent,), jnp.int32),
            pltpu.SMEM((SLOTS,), jnp.int32),
        ],
        compiler_params=pltpu.CompilerParams(vmem_limit_bytes=NEAR_VMEM),
        cost_estimate=pl.CostEstimate(flops=10**9, bytes_accessed=10**7, transcendentals=10**7),
        name="near_field",
    )(place, halo_c, own_c, rel, halo_x, halo_p, own_x, own_p, far)


MESH = pl.DeviceIdType.MESH
HALF = 64
PIECES = 4
FAR_VMEM = 48 * 1024 * 1024
NT = (((1,), (1,)), ((), ()))
NN = (((1,), (0,)), ((), ()))


def split(x):
    high = x.astype(jnp.bfloat16)
    return high, (x - high.astype(jnp.float32)).astype(jnp.bfloat16)


def dot(a, b, dims):
    return lax.dot_general(a, b, dims, preferred_element_type=jnp.float32)


def dot_split(a, b, dims):
    a_high, a_low = split(a)
    b_high, b_low = split(b)
    rows = a.shape[0]
    both = dot(jnp.concatenate([a_high, a_low], axis=0), b_high, dims)
    return both[:rows] + both[rows:] + dot(a_high, b_low, dims)


def swap(x):
    return pltpu.roll(x, HALF, 1)


def fold(x):
    lane = lax.broadcasted_iota(jnp.int32, (16, LANES), 1)
    return jnp.where(lane < HALF, x[:16], x[16:])


def far_kernel(
    shape,
    count_smem, parent, box_parent, far1, far2,
    points, rhs, basis, transfer, nodes, box_transfer, nodes2, counts,
    halo_x, halo_p, halo_c, g_out,
    x_v, basis_v, transfer_v, m1, acc, part, partial, m2, own_n, own_n2, all_n2,
    load_sems, halo_send, halo_recv, x_send, x_recv, y_send, y_recv, r_send, r_recv, d_send, d_recv, z_send, z_recv,
):
    n_grp, n_dev, n_x = shape
    grp, dev = lax.axis_index("grp"), lax.axis_index("dev")
    n_y = n_dev // n_x
    my_y, my_x = dev // n_x, lax.rem(dev, n_x)
    leaves = parent.shape[0]
    boxes = box_parent.shape[0]
    reach = halo_x.shape[2]
    units = boxes + boxes // 4
    lane = lax.broadcasted_iota(jnp.int32, (R, LANES), 1)
    low = lane < HALF

    loads = [
        pltpu.make_async_copy(rhs, x_v, load_sems.at[0]),
        pltpu.make_async_copy(basis, basis_v, load_sems.at[1]),
        pltpu.make_async_copy(transfer, transfer_v, load_sems.at[2]),
    ]
    for copy in loads:
        copy.start()

    barrier = pltpu.get_barrier_semaphore()
    for step in range(1, n_dev):
        pl.semaphore_signal(barrier, inc=1, device_id={"dev": lax.rem(dev + step, n_dev)}, device_id_type=MESH)
    for step in range(1, n_grp):
        pl.semaphore_signal(barrier, inc=1, device_id={"grp": lax.rem(grp + step, n_grp)}, device_id_type=MESH)
    pl.semaphore_wait(barrier, n_dev - 1 + n_grp - 1)

    def remote(src, dst, send, recv, **place):
        return pltpu.make_async_remote_copy(
            src_ref=src, dst_ref=dst, send_sem=send, recv_sem=recv, device_id=place, device_id_type=MESH
        )

    width = x_v.shape[1]
    part_w = reach // PIECES
    halo = []
    for side in range(2):
        to = lax.rem(dev + (1 if side == 0 else n_dev - 1), n_dev)
        first = width - reach if side == 0 else 0
        for piece in range(PIECES):
            halo.append(
                remote(
                    rhs.at[:, pl.ds(first + piece * part_w, part_w)],
                    halo_x.at[side, :, pl.ds(piece * part_w, part_w)],
                    halo_send.at[side, piece],
                    halo_recv.at[side, piece],
                    dev=to,
                )
            )
        halo.append(
            remote(points.at[:, pl.ds(first, reach)], halo_p.at[side], halo_send.at[side, PIECES], halo_recv.at[side, PIECES], dev=to)
        )
        halo.append(
            remote(counts.at[0], halo_c.at[2 * side], halo_send.at[side, PIECES + 1], halo_recv.at[side, PIECES + 1], dev=to)
        )
    per = PIECES + 2

    def start_halo(which):
        for side in range(2):
            for i in which:
                halo[side * per + i].start()

    start_halo([PIECES, PIECES + 1, 0])

    acc[...] = jnp.zeros_like(acc)
    loads[0].wait()
    loads[1].wait()
    loads[2].wait()
    slot = lax.broadcasted_iota(jnp.int32, (R, B), 1)

    def lift(p, carry):
        expansions = []
        for i in range(2):
            c = 2 * p + i
            at = pl.ds(pl.multiple_of(c * B, B), B)
            x = jnp.where(slot < count_smem[c], x_v[:, at], 0.0)
            x_high, x_low = split(x)
            b_high, b_low = split(basis_v[:, at])
            both = dot(jnp.concatenate([x_high, x_low], axis=0), jnp.concatenate([b_high, b_low], axis=0), NT)
            top, bottom = both[:R], both[R:]
            expansions.append((top + bottom + swap(top))[:, :HALF])
        slab = transfer_v[:, pl.ds(pl.multiple_of(p * LANES, LANES), LANES)]
        out = dot_split(jnp.concatenate(expansions, axis=0), slab, NN)
        value = jnp.where(low, out[:R], out[R:])
        owner = jnp.where(low, parent[2 * p], parent[2 * p + 1]) - (grp * n_dev + dev) * boxes
        for b in range(boxes):
            acc[b] += jnp.where(owner == b, value, 0.0)
        return carry

    lax.fori_loop(0, leaves // 2, lift, 0, unroll=2)

    for b in range(boxes):
        full = acc[b] + swap(acc[b])
        acc[b] = full
        m1[dev * units + b] = fold(full)
    for q in range(boxes // 2):
        row = q % 2 * 8
        m1[dev * units + boxes + q // 2, row : row + 3, :] = nodes[:, q * LANES : (q + 1) * LANES]
    own_block = m1.at[pl.ds(dev * units, units)]
    x_copies = []
    for step in range(1, n_x):
        to = my_y * n_x + lax.rem(my_x + step, n_x)
        copy = remote(own_block, own_block, x_send.at[step - 1], x_recv.at[step - 1], dev=to)
        copy.start()
        x_copies.append(copy)

    sums = [jnp.zeros((16, LANES), jnp.float32) for _ in range(n_dev)]
    for q in range(boxes // 2):
        pair = jnp.concatenate([acc[2 * q], acc[2 * q + 1]], axis=0)[:, :HALF]
        out = dot_split(pair, box_transfer[:, q * LANES : (q + 1) * LANES], NN)
        for i in range(2):
            half = jnp.where(low == (i == 0), out[i * R : (i + 1) * R], 0.0)
            folded = fold(half + swap(half))
            owner = box_parent[2 * q + i] - grp * n_dev
            for p in range(n_dev):
                sums[p] += jnp.where(owner == p, folded, 0.0)
    for p in range(n_dev):
        partial[p] = sums[p]
    r_copies = []
    for step in range(1, n_dev):
        to = lax.rem(dev + step, n_dev)
        copy = remote(partial.at[to], part.at[step - 1], r_send.at[step - 1], r_recv.at[step - 1], dev=to)
        copy.start()
        r_copies.append(copy)
    start_halo([1])

    for q in range(boxes // 2):
        own_n[q * LANES : (q + 1) * LANES, :] = (
            jnp.concatenate([nodes[:, q * LANES : (q + 1) * LANES], jnp.zeros((5, LANES), jnp.float32)], axis=0) * 4.0
        ).T
    for q in range(n_dev // 2):
        at = pl.ds(pl.multiple_of((grp * n_dev // 2 + q) * LANES, LANES), LANES)
        flipped = (jnp.concatenate([nodes2[:, at], jnp.zeros((5, LANES), jnp.float32)], axis=0) * 4.0).T
        own_n2[2 * q] = flipped[:K]
        own_n2[2 * q + 1] = flipped[K:]

    def spread_nodes(q, carry):
        all_n2[q, 0:3, :] = nodes2[:, pl.ds(pl.multiple_of(q * LANES, LANES), LANES)]
        return carry

    lax.fori_loop(0, nodes2.shape[1] // LANES, spread_nodes, 0, unroll=8)

    total = partial[dev]
    for step in range(1, n_dev):
        r_copies[step - 1].wait_recv()
        total += part[step - 1]
    m2[grp, dev] = total
    d_copies = []
    for step in range(1, n_dev):
        to = lax.rem(dev + step, n_dev)
        copy = remote(m2.at[grp, dev], m2.at[grp, dev], d_send.at[step - 1], d_recv.at[step - 1], dev=to)
        copy.start()
        d_copies.append(copy)
    for copy in x_copies:
        copy.wait_recv()
    y_copies = []
    for step in range(1, n_y):
        to = lax.rem(my_y + step, n_y) * n_x + my_x
        row_block = m1.at[pl.ds(my_y * n_x * units, n_x * units)]
        copy = remote(row_block, row_block, y_send.at[step - 1], y_recv.at[step - 1], dev=to)
        copy.start()
        y_copies.append(copy)
    start_halo(range(2, PIECES))
    for copy in d_copies:
        copy.wait_recv()
    z_copies = []
    for step in range(1, n_grp):
        to = lax.rem(grp + step, n_grp)
        copy = remote(m2.at[grp], m2.at[grp], z_send.at[step - 1], z_recv.at[step - 1], grp=to)
        copy.start()
        z_copies.append(copy)

    def couple(own, sources):
        spread = [jnp.broadcast_to(own[:, d : d + 1], (K, LANES)) for d in range(3)]
        total = jnp.zeros((R, K), jnp.float32)
        for first in range(0, len(sources), 4):
            highs, lows, parts = [], [], []
            for i in range(first, first + 4, 2):
                (v0, n0, odd0), (v1, n1, odd1) = sources[i], sources[i + 1]
                value = jnp.where(
                    low, jnp.concatenate([v0, swap(v0)], axis=0), jnp.concatenate([swap(v1), v1], axis=0)
                )
                n0 = jnp.where(odd0, swap(n0), n0)
                n1 = jnp.where(odd1, n1, swap(n1))
                place = jnp.where(low[:3], n0, n1) * 4.0
                d0, d1, d2 = (spread[d] - place[d : d + 1] for d in range(3))
                high, rest = split(lax.rsqrt(((1.0 + d0 * d0) + d1 * d1) + d2 * d2))
                highs.append(high)
                lows.append(rest)
                parts.append(value)
            value = jnp.concatenate(parts, axis=1)
            value_high, value_low = split(value)
            high, rest = jnp.concatenate(highs, axis=1), jnp.concatenate(lows, axis=1)
            both = dot(jnp.concatenate([value_high, value_low], axis=0), high, NT)
            total += both[:R] + both[R:] + dot(value_high, rest, NT)
        return total

    for copy in y_copies:
        copy.wait_recv()

    def level_one(t, carry):
        sources = []
        for i in range(far1.shape[1]):
            s = lax.rem(far1[t, i], n_dev * boxes)
            home, box = lax.div(s, boxes), lax.rem(s, boxes)
            v = m1[home * units + box]
            both = m1[home * units + boxes + lax.div(box, 4)]
            n = jnp.where(lax.rem(lax.div(box, 2), 2) == 1, both[8:11], both[0:3])
            sources.append((v, n, lax.rem(box, 2) == 1))
        own = own_n[pl.ds(pl.multiple_of(t * K, K), K), :]
        acc[t, :, 0:HALF] = couple(own, sources)
        return carry

    lax.fori_loop(0, boxes, level_one, 0)

    for copy in z_copies:
        copy.wait_recv()

    def level_two(t, carry):
        target = box_parent[t]
        sources = []
        for i in range(far2.shape[1]):
            s = far2[target, i]
            v = m2[lax.div(s, n_dev), lax.rem(s, n_dev)]
            n = all_n2[lax.div(s, 2)][:3]
            sources.append((v, n, lax.rem(s, 2) == 1))
        own = own_n2[lax.rem(target, n_dev)]
        acc[t, :, HALF:LANES] = couple(own, sources)
        return carry

    lax.fori_loop(0, boxes, level_two, 0)

    for q in range(boxes // 2):
        rows = []
        for i in range(2):
            coarse = acc[2 * q + i]
            rows.append(jnp.where(low, swap(coarse), 0.0) if i == 0 else jnp.where(low, 0.0, coarse))
        moved = dot_split(jnp.concatenate(rows, axis=0), box_transfer[:, q * LANES : (q + 1) * LANES], NT)
        for i in range(2):
            g = acc[2 * q + i][:, :HALF] + moved[i * R : (i + 1) * R]
            g_out[2 * q + i] = jnp.concatenate([g, g], axis=1)

    for copies in (x_copies, r_copies, d_copies, y_copies, z_copies):
        for copy in copies:
            copy.wait_send()
    for copy in halo:
        copy.wait()


def far_field(mesh_shape, count, parent, box_parent, far1, far2, points, rhs, basis, transfer, nodes, box_transfer, nodes2):
    n_grp, n_dev, n_x = mesh_shape
    boxes = box_parent.shape[0]
    reach = REACH * B
    width = rhs.shape[1]
    vmem = pl.BlockSpec(memory_space=pltpu.VMEM)
    smem = pl.BlockSpec(memory_space=pltpu.SMEM)
    hbm = pl.BlockSpec(memory_space=pl.ANY)
    dma = pltpu.SemaphoreType.DMA
    units = boxes + boxes // 4
    return pl.pallas_call(
        functools.partial(far_kernel, mesh_shape),
        out_shape=(
            jax.ShapeDtypeStruct((2, R, reach), jnp.float32),
            jax.ShapeDtypeStruct((2, 3, reach), jnp.float32),
            jax.ShapeDtypeStruct((3, 1, count.shape[0]), jnp.int32),
            jax.ShapeDtypeStruct((boxes, R, LANES), jnp.float32),
        ),
        in_specs=[smem] * 5 + [hbm, hbm, hbm, hbm, vmem, vmem, vmem, vmem],
        out_specs=(hbm, hbm, vmem, vmem),
        scratch_shapes=[
            pltpu.VMEM((R, width), jnp.float32),
            pltpu.VMEM((K, width), jnp.float32),
            pltpu.VMEM(transfer.shape, jnp.float32),
            pltpu.VMEM((n_dev * units, 16, LANES), jnp.float32),
            pltpu.VMEM((boxes, R, LANES), jnp.float32),
            pltpu.VMEM((n_dev - 1, 16, LANES), jnp.float32),
            pltpu.VMEM((n_dev, 16, LANES), jnp.float32),
            pltpu.VMEM((n_grp, n_dev, 16, LANES), jnp.float32),
            pltpu.VMEM((boxes * K, 8), jnp.float32),
            pltpu.VMEM((n_dev, K, 8), jnp.float32),
            pltpu.VMEM((nodes2.shape[1] // LANES, 8, LANES), jnp.float32),
            dma((3,)),
            dma((2, PIECES + 2)), dma((2, PIECES + 2)),
            dma((n_x - 1,)), dma((n_x - 1,)),
            dma((n_dev // n_x - 1,)), dma((n_dev // n_x - 1,)),
            dma((n_dev - 1,)), dma((n_dev - 1,)),
            dma((n_dev - 1,)), dma((n_dev - 1,)),
            dma((n_grp - 1,)), dma((n_grp - 1,)),
        ],
        compiler_params=pltpu.CompilerParams(collective_id=0, has_side_effects=True, vmem_limit_bytes=FAR_VMEM),
        cost_estimate=pl.CostEstimate(flops=10**9, bytes_accessed=10**7, transcendentals=10**6),
        name="far_field",
    )(count, parent, box_parent, far1, far2, points, rhs, basis, transfer, nodes, box_transfer, nodes2, count.reshape(1, 1, -1))


def down_kernel(parent, first_box, g, transfer, basis, out):
    low = lax.broadcasted_iota(jnp.int32, (R, LANES), 1) < HALF

    def one(p, carry):
        top = g[parent[2 * p] - first_box[0]]
        bottom = g[parent[2 * p + 1] - first_box[0]]
        rows = jnp.concatenate([jnp.where(low, top, 0.0), jnp.where(low, 0.0, bottom)], axis=0)
        slab = transfer[:, pl.ds(pl.multiple_of(p * LANES, LANES), LANES)]
        moved = dot_split(rows, slab, NT)
        high, rest = split(moved)
        left = jnp.concatenate([high, rest, high], axis=1)
        for i in range(2):
            at = pl.ds(pl.multiple_of((2 * p + i) * B, B), B)
            b_high, b_low = split(basis[:, at])
            out[:, at] = dot(left[i * R : (i + 1) * R], jnp.concatenate([b_high, b_high, b_low], axis=0), NN)
        return carry

    lax.fori_loop(0, parent.shape[0] // 2, one, 0, unroll=2)


def down(parent, first_box, g, transfer, basis):
    vmem = pl.BlockSpec(memory_space=pltpu.VMEM)
    smem = pl.BlockSpec(memory_space=pltpu.SMEM)
    return pl.pallas_call(
        down_kernel,
        out_shape=jax.ShapeDtypeStruct((R, basis.shape[1]), jnp.float32),
        in_specs=[smem, smem, vmem, vmem, vmem],
        out_specs=vmem,
        compiler_params=pltpu.CompilerParams(vmem_limit_bytes=FAR_VMEM),
        cost_estimate=pl.CostEstimate(flops=10**8, bytes_accessed=10**7, transcendentals=0),
        name="down",
    )(parent, first_box, g, transfer, basis)


def local(
    mesh_shape,
    points,
    rhs,
    leaf_count,
    near_list,
    leaf_basis,
    leaf_transfer,
    leaf_parent,
    nodes1,
    box_transfer,
    box_parent,
    far1,
    nodes2,
    far2,
):
    leaves = leaf_count.shape[0]
    boxes = box_parent.shape[0]
    device = lax.axis_index("grp") * lax.axis_size("dev") + lax.axis_index("dev")
    halo_x, halo_p, halo_c, g = far_field(
        mesh_shape, leaf_count, leaf_parent, box_parent, far1, far2,
        points, rhs, leaf_basis, leaf_transfer, nodes1, box_transfer, nodes2,
    )
    place = jnp.stack([device * boxes, device * leaves - REACH])
    far = down(leaf_parent, place, g, leaf_transfer, leaf_basis)
    return near_field(place, halo_c, leaf_count, near_list, halo_x, halo_p, rhs, points, far)


def solution(mesh):
    placed = (
        P(None, ("grp", "dev")),
        P(None, ("grp", "dev")),
        P(("grp", "dev")),
        P(("grp", "dev"), None),
        P(None, ("grp", "dev")),
        P(None, ("grp", "dev")),
        P(("grp", "dev")),
        P(None, ("grp", "dev")),
        P(None, ("grp", "dev")),
        P(("grp", "dev")),
        P(("grp", "dev"), None),
        P(),
        P(),
    )
    mesh_shape = (mesh.shape["grp"], mesh.shape["dev"], 4)
    return jax.shard_map(
        functools.partial(local, mesh_shape),
        mesh=mesh, in_specs=placed, out_specs=P(None, ("grp", "dev")), check_vma=False
    )
```

```python
import functools

import jax
import jax.numpy as jnp
from jax import lax
from jax.experimental import pallas as pl
from jax.experimental.pallas import tpu as pltpu
from jax.sharding import PartitionSpec as P

B = 256
K = 64
R = 32
NEAR = 8
REACH = 32
LANES = 128
TILE = 32
SLOTS = 2
NEAR_VMEM = 56 * 1024 * 1024


def near_kernel(leaves, place, halo_c, own_c, rel, halo_x, halo_p, own_x, own_p, far, out, xs, pb, ab, sums, lists, cnt, bases, turns, accs):
    halo = halo_x.shape[2] // B
    total = leaves + 2 * halo
    for i in range(halo):
        cnt[i] = halo_c[0, 0, leaves - halo + i]
        cnt[halo + leaves + i] = halo_c[2, 0, i]
    for i in range(leaves):
        cnt[halo + i] = own_c[i]
    lane = lax.broadcasted_iota(jnp.int32, (R, B), 1)

    def load_source(src_x, src_p, first, i):
        at = pl.ds(pl.multiple_of(i * B, B), B)
        to = pl.ds(pl.multiple_of((first + i) * B, B), B)
        x = jnp.where(lane < cnt[first + i], src_x[:, at], 0.0)
        high = x.astype(jnp.bfloat16)
        xs[0:R, to] = high
        xs[R : 2 * R, to] = (x - high.astype(jnp.float32)).astype(jnp.bfloat16)
        scaled = src_p[:, at] * 4.0
        pb[0:3, to] = scaled
        return scaled

    def load_halo(i, carry):
        load_source(halo_x.at[0], halo_p.at[0], 0, i)
        load_source(halo_x.at[1], halo_p.at[1], halo + leaves, i)
        return carry

    lax.fori_loop(0, halo, load_halo, 0, unroll=2)
    tail = pl.ds(total * B, 2 * LANES)
    xs[:, tail] = jnp.zeros((2 * R, 2 * LANES), jnp.bfloat16)
    pb[:, tail] = jnp.zeros((8, 2 * LANES), jnp.float32)

    def load_own(i, start):
        scaled = load_source(own_x, own_p, halo, i)
        padded = jnp.concatenate([scaled, jnp.zeros((5, B), jnp.float32)], axis=0)
        for half in range(B // LANES):
            flipped = padded[:, half * LANES : (half + 1) * LANES].T
            for d in range(3):
                ab[i, d, half * LANES : (half + 1) * LANES, :] = jnp.broadcast_to(
                    flipped[:, d : d + 1], (LANES, LANES)
                )
        at = start
        for n in range(NEAR):
            src = rel[n, i] - place[1]
            lists[at] = 2 * src
            lists[at + 1] = 2 * src + 1
            at = at + 1 + (cnt[src] > LANES).astype(jnp.int32)
        lists[at] = 2 * total
        chunks = (at - start + 1) // 2
        at = start + 2 * chunks
        lists[at] = lists[at - 2]
        lists[at + 1] = lists[at - 1]
        bases[i] = start
        turns[i] = chunks
        return start + 4 * ((chunks + 1) // 2)

    end = lax.fori_loop(0, leaves, load_own, 0, unroll=2)
    for i in range(4):
        lists[end + i] = 2 * total

    def push(start):
        for unit in range(2):
            parts = []
            for half in range(2):
                at = lists[start + 2 * unit + half]
                parts.append(xs[:, pl.ds(pl.multiple_of(at * LANES, LANES), LANES)])
            w = jnp.concatenate(parts, axis=1)
            pltpu.matmul_push_rhs(jnp.concatenate([w] * 4, axis=0), 0, unit, transpose=True)

    def pop(slot, target):
        for t in range(B // TILE):
            both = pltpu.matmul_pop(accs[0][slot][t]) + pltpu.matmul_pop(accs[1][slot][t])
            sums[target, t * TILE : (t + 1) * TILE, :] = both[:, :LANES]

    def couple_step(slot, tiles, target, start, split_rows):
        cols = []
        for unit in range(1 if split_rows else 2):
            halves = []
            for half in range(2):
                at = lists[start + 2 * unit + half]
                at = pl.ds(pl.multiple_of(at * LANES, LANES), LANES)
                halves.append([pb[d : d + 1, at] for d in range(3)])
            cols.append(halves)
        fresh = [True, True]
        waiting = [[], []]
        for t in range(tiles):
            own = [ab[target, d, t * TILE : (t + 1) * TILE, :] for d in range(3)]
            for unit in [t % 2] if split_rows else range(2):
                highs, lows = [], []
                for half in range(2):
                    col = cols[0 if split_rows else unit][half]
                    d0, d1, d2 = (own[d] - col[d] for d in range(3))
                    k = lax.rsqrt(((1.0 + d0 * d0) + d1 * d1) + d2 * d2)
                    high = k.astype(jnp.bfloat16)
                    highs.append(high)
                    lows.append((k - high.astype(jnp.float32)).astype(jnp.bfloat16))
                acc = accs[unit][slot][t]
                pltpu.matmul_acc_lhs(acc, jnp.concatenate(highs, axis=1), load_staged_rhs=0 if fresh[unit] else None)
                fresh[unit] = False
                for args in waiting[unit]:
                    pltpu.matmul_acc_lhs(*args)
                waiting[unit] = [(acc, jnp.concatenate(lows, axis=1))]
            if t == (1 if split_rows else 0):
                push(start + 4)
        for unit in range(2):
            for args in waiting[unit]:
                pltpu.matmul_acc_lhs(*args)

    def sweep(slot, tiles, target):
        start, count = bases[target], turns[target]

        def pair(i, carry):
            couple_step(slot, tiles, target, start + 4 * i, False)
            return carry

        lax.fori_loop(0, lax.div(count, 2), pair, 0)

        @pl.when(lax.rem(count, 2) == 1)
        def _():
            couple_step(slot, tiles, target, start + 2 * (count - 1), True)

    for slot in range(SLOTS):
        pop(slot, leaves)
    push(0)

    def group(g, carry):
        for slot in range(SLOTS):
            target = SLOTS * g + slot
            kind = lax.div(cnt[halo + target] + (TILE - 1), TILE) - 2
            lax.switch(kind, [functools.partial(sweep, slot, tiles, target) for tiles in range(2, B // TILE + 1)])
            pop(1 - slot, jnp.where(target == 0, leaves, target - 1))
        return carry

    lax.fori_loop(0, leaves // SLOTS, group, 0)
    for unit in range(2):
        pltpu.matmul_acc_lhs(accs[unit][0][0], jnp.zeros((TILE, 2 * LANES), jnp.bfloat16), load_staged_rhs=0)
    pop(1, leaves - 1)
    pop(0, leaves)

    def finish(target, carry):
        parts = []
        for half in range(B // LANES):
            flipped = sums[target, half * LANES : (half + 1) * LANES, :].T
            parts.append(flipped[0:R] + flipped[R : 2 * R])
        at = pl.ds(pl.multiple_of(target * B, B), B)
        value = jnp.concatenate(parts, axis=1) + far[:, at]
        out[:, at] = jnp.where(lane < cnt[halo + target], value, 0.0)
        return carry

    lax.fori_loop(0, leaves, finish, 0, unroll=4)


def near_body(leaves, *refs):
    tiles = B // TILE
    specs = tuple(
        tuple(tuple(pltpu.ACC(unit)((TILE, 256), jnp.float32) for _ in range(tiles)) for _ in range(SLOTS))
        for unit in range(2)
    )
    pl.run_scoped(lambda accs: near_kernel(leaves, *refs, accs), specs)


def near_field(place, halo_c, own_c, rel, halo_x, halo_p, own_x, own_p, far):
    leaves = own_x.shape[1] // B
    extent = leaves + 2 * (halo_x.shape[2] // B)
    wide = extent * B + 2 * LANES
    vmem = pl.BlockSpec(memory_space=pltpu.VMEM)
    smem = pl.BlockSpec(memory_space=pltpu.SMEM)
    return pl.pallas_call(
        functools.partial(near_body, leaves),
        out_shape=jax.ShapeDtypeStruct((R, leaves * B), jnp.float32),
        in_specs=[smem] * 4 + [vmem] * 5,
        out_specs=vmem,
        scratch_shapes=[
            pltpu.VMEM((2 * R, wide), jnp.bfloat16),
            pltpu.VMEM((8, wide), jnp.float32),
            pltpu.VMEM((leaves, 3, B, LANES), jnp.float32),
            pltpu.VMEM((leaves + 1, B, LANES), jnp.float32),
            pltpu.SMEM((leaves * 16 + 24,), jnp.int32),
            pltpu.SMEM((extent,), jnp.int32),
            pltpu.SMEM((leaves,), jnp.int32),
            pltpu.SMEM((leaves,), jnp.int32),
        ],
        compiler_params=pltpu.CompilerParams(vmem_limit_bytes=NEAR_VMEM),
        cost_estimate=pl.CostEstimate(flops=10**9, bytes_accessed=10**7, transcendentals=10**7),
        name="near_field",
    )(place, halo_c, own_c, rel, halo_x, halo_p, own_x, own_p, far)


MESH = pl.DeviceIdType.MESH
HALF = 64
PIECES = 8
FIRST_PIECES = 1
HALO_FIRST = 0
ALONG_X = (True, False)
FAR_VMEM = 62 * 1024 * 1024
NT = (((1,), (1,)), ((), ()))
NN = (((1,), (0,)), ((), ()))


def split(x):
    high = x.astype(jnp.bfloat16)
    return high, (x - high.astype(jnp.float32)).astype(jnp.bfloat16)


def dot(a, b, dims):
    return lax.dot_general(a, b, dims, preferred_element_type=jnp.float32)


def dot_split(a, b, dims):
    a_high, a_low = split(a)
    b_high, b_low = split(b)
    rows = a.shape[0]
    both = dot(jnp.concatenate([a_high, a_low], axis=0), b_high, dims)
    return both[:rows] + both[rows:] + dot(a_high, b_low, dims)


def swap(x):
    return pltpu.roll(x, HALF, 1)


def fold(x):
    lane = lax.broadcasted_iota(jnp.int32, (16, LANES), 1)
    return jnp.where(lane < HALF, x[:16], x[16:])


def far_kernel(
    shape,
    count_h, parent_h, box_parent_h, far1_h, far2_h,
    points, rhs, basis, transfer, nodes_h, box_transfer_h, nodes2_h, counts,
    halo_x, halo_p, halo_c, far_out,
    count, parent, box_parent, far1, far2, nodes, box_transfer, nodes2,
    x_v, basis_v, transfer_v, m1, near_nodes, acc, g1, part, partial, m2, own_n, own_n2, all_n2, expanded, spread_g,
    load_sems, halo_send, halo_recv, n_send, n_recv, a_send, a_recv, b_send, b_recv,
    r_send, r_recv, d_send, d_recv, z_send, z_recv, c_send, c_recv,
):
    n_grp, n_dev, n_x = shape
    grp, dev = lax.axis_index("grp"), lax.axis_index("dev")
    n_y = n_dev // n_x
    my_y, my_x = dev // n_x, lax.rem(dev, n_x)
    leaves = parent.shape[0]
    boxes = box_parent.shape[0]
    reach = halo_x.shape[2]
    half_boxes = boxes // 2
    low = lax.broadcasted_iota(jnp.int32, (R, LANES), 1) < HALF

    pairs = [
        (nodes_h, nodes), (count_h, count), (parent_h, parent), (rhs, x_v), (basis, basis_v), (transfer, transfer_v),
        (box_parent_h, box_parent), (box_transfer_h, box_transfer), (far1_h, far1), (far2_h, far2), (nodes2_h, nodes2),
    ]
    loads = [pltpu.make_async_copy(src, dst, load_sems.at[i]) for i, (src, dst) in enumerate(pairs)]
    for copy in loads:
        copy.start()

    barrier = pltpu.get_barrier_semaphore()
    for step in range(1, n_dev):
        pl.semaphore_signal(barrier, inc=1, device_id={"dev": lax.rem(dev + step, n_dev)}, device_id_type=MESH)
    for to in [lax.rem(grp + 2 * step, n_grp) for step in range(1, n_grp // 2)] + [grp + 1 - 2 * lax.rem(grp, 2)]:
        pl.semaphore_signal(barrier, inc=1, device_id={"grp": to}, device_id_type=MESH)
    pl.semaphore_wait(barrier, n_dev - 1 + n_grp // 2)

    def remote(src, dst, send, recv, **place):
        return pltpu.make_async_remote_copy(
            src_ref=src, dst_ref=dst, send_sem=send, recv_sem=recv, device_id=place, device_id_type=MESH
        )

    width = x_v.shape[1]
    part_w = reach // PIECES
    halo = []
    for side in range(2):
        to = lax.rem(dev + (1 if side == 0 else n_dev - 1), n_dev)
        first = width - reach if side == 0 else 0
        for piece in range(PIECES):
            halo.append(
                remote(
                    rhs.at[:, pl.ds(first + piece * part_w, part_w)],
                    halo_x.at[side, :, pl.ds(piece * part_w, part_w)],
                    halo_send.at[side, piece],
                    halo_recv.at[side, piece],
                    dev=to,
                )
            )
        halo.append(
            remote(points.at[:, pl.ds(first, reach)], halo_p.at[side], halo_send.at[side, PIECES], halo_recv.at[side, PIECES], dev=to)
        )
        halo.append(
            remote(counts.at[0], halo_c.at[2 * side], halo_send.at[side, PIECES + 1], halo_recv.at[side, PIECES + 1], dev=to)
        )
    per = PIECES + 2
    sends = (dev < n_dev - 1, dev > 0)

    def start_halo(which):
        for side in range(2):

            @pl.when(sends[side])
            def _():
                for i in which:
                    halo[side * per + i].start()

    loads[0].wait()
    for q in range(half_boxes):
        near_nodes[dev * (half_boxes // 2) + q // 2, q % 2 * 8 : q % 2 * 8 + 3, :] = nodes[:, q * LANES : (q + 1) * LANES]
    own_nodes = near_nodes.at[pl.ds(dev * (half_boxes // 2), half_boxes // 2)]
    n_copies = []
    for step in range(1, n_dev):
        to = lax.rem(dev + step, n_dev)
        copy = remote(own_nodes, own_nodes, n_send.at[step - 1], n_recv.at[step - 1], dev=to)
        copy.start()
        n_copies.append(copy)
    start_halo([PIECES, PIECES + 1] + list(range(FIRST_PIECES)))

    acc[...] = jnp.zeros_like(acc)
    for copy in loads[1:]:
        copy.wait()
    slot = lax.broadcasted_iota(jnp.int32, (R, B), 1)

    def expand(p, carry):
        for i in range(2):
            c = 2 * p + i
            at = pl.ds(pl.multiple_of(c * B, B), B)
            x = jnp.where(slot < count[c], x_v[:, at], 0.0)
            x_high, x_low = split(x)
            b_high, b_low = split(basis_v[:, at])
            both = dot(jnp.concatenate([x_high, x_low], axis=0), jnp.concatenate([b_high, b_low], axis=0), NT)
            top, bottom = both[:R], both[R:]
            expanded[p, i * R : (i + 1) * R, :] = top + bottom + swap(top)
        return carry

    lax.fori_loop(0, leaves // 2, expand, 0, unroll=4)

    def lift(p, carry):
        slab = transfer_v[:, pl.ds(pl.multiple_of(p * LANES, LANES), LANES)]
        out = dot_split(expanded[p][:, :HALF], slab, NN)
        value = jnp.where(low, out[:R], out[R:])
        owner = jnp.where(low, parent[2 * p], parent[2 * p + 1]) - (grp * n_dev + dev) * boxes
        for b in range(boxes):
            acc[b] += jnp.where(owner == b, value, 0.0)
        return carry

    lax.fori_loop(0, leaves // 2, lift, 0, unroll=4)

    for b in range(boxes):
        full = acc[b] + swap(acc[b])
        acc[b] = full
        m1[b // half_boxes, dev * half_boxes + b % half_boxes] = fold(full)
    first, second = [], []

    def along(which, block, to, sem, copies):
        copy = remote(block, block, a_send.at[which, sem], a_recv.at[which, sem], dev=to)
        copy.start()
        copies.append(copy)

    mine = [m1.at[i, pl.ds(dev * half_boxes, half_boxes)] for i in range(2)]
    for which, along_x in enumerate(ALONG_X):
        for step in range(1, n_x if along_x else n_y):
            to = my_y * n_x + lax.rem(my_x + step, n_x) if along_x else lax.rem(my_y + step, n_y) * n_x + my_x
            along(which, mine[which], to, step - 1, first)

    sums = [jnp.zeros((16, LANES), jnp.float32) for _ in range(n_dev)]
    for q in range(boxes // 2):
        pair = jnp.concatenate([acc[2 * q], acc[2 * q + 1]], axis=0)[:, :HALF]
        out = dot_split(pair, box_transfer[:, q * LANES : (q + 1) * LANES], NN)
        for i in range(2):
            half = jnp.where(low == (i == 0), out[i * R : (i + 1) * R], 0.0)
            folded = fold(half + swap(half))
            owner = box_parent[2 * q + i] - grp * n_dev
            for p in range(n_dev):
                sums[p] += jnp.where(owner == p, folded, 0.0)
    for p in range(n_dev):
        partial[p] = sums[p]
    r_copies = []
    for step in range(1, n_dev):
        to = lax.rem(dev + step, n_dev)
        copy = remote(partial.at[to], part.at[step - 1], r_send.at[step - 1], r_recv.at[step - 1], dev=to)
        copy.start()
        r_copies.append(copy)
    start_halo(range(FIRST_PIECES, FIRST_PIECES + 1))

    for q in range(boxes // 2):
        own_n[q * LANES : (q + 1) * LANES, :] = (
            jnp.concatenate([nodes[:, q * LANES : (q + 1) * LANES], jnp.zeros((5, LANES), jnp.float32)], axis=0) * 4.0
        ).T
    for q in range(n_dev // 2):
        at = pl.ds(pl.multiple_of((grp * n_dev // 2 + q) * LANES, LANES), LANES)
        flipped = (jnp.concatenate([nodes2[:, at], jnp.zeros((5, LANES), jnp.float32)], axis=0) * 4.0).T
        own_n2[2 * q] = flipped[:K]
        own_n2[2 * q + 1] = flipped[K:]

    def spread_nodes(q, carry):
        all_n2[q, 0:3, :] = nodes2[:, pl.ds(pl.multiple_of(q * LANES, LANES), LANES)]
        return carry

    lax.fori_loop(0, nodes2.shape[1] // LANES, spread_nodes, 0, unroll=8)

    total = partial[dev]
    for step in range(1, n_dev):
        r_copies[step - 1].wait_recv()
        total += part[step - 1]
    m2[grp, dev] = total
    d_copies = []
    for step in range(1, n_dev):
        to = lax.rem(dev + step, n_dev)
        copy = remote(m2.at[grp, dev], m2.at[grp, dev], d_send.at[step - 1], d_recv.at[step - 1], dev=to)
        copy.start()
        d_copies.append(copy)
    for copy in first:
        copy.wait_recv()
    if HALO_FIRST:
        start_halo(range(FIRST_PIECES + 1, HALO_FIRST))
    for which, along_x in enumerate(ALONG_X):
        for step in range(1, n_y if along_x else n_x):
            if along_x:
                row = m1.at[which, pl.ds(my_y * n_x * half_boxes, n_x * half_boxes)]
                to = lax.rem(my_y + step, n_y) * n_x + my_x
                copy = remote(row, row, b_send.at[which, step - 1, 0], b_recv.at[which, step - 1, 0], dev=to)
                copy.start()
                second.append(copy)
            else:
                for y in range(n_y):
                    piece = m1.at[which, pl.ds((y * n_x + my_x) * half_boxes, half_boxes)]
                    to = my_y * n_x + lax.rem(my_x + step, n_x)
                    copy = remote(piece, piece, b_send.at[which, step - 1, y], b_recv.at[which, step - 1, y], dev=to)
                    copy.start()
                    second.append(copy)
    start_halo(range(max(FIRST_PIECES + 1, HALO_FIRST), PIECES))
    for copy in d_copies:
        copy.wait_recv()
    other = grp + 1 - 2 * lax.rem(grp, 2)
    z_copies, c_copies = [], []
    for step in range(1, n_grp // 2):
        to = lax.rem(grp + 2 * step, n_grp)
        copy = remote(m2.at[grp], m2.at[grp], z_send.at[step - 1], z_recv.at[step - 1], grp=to)
        copy.start()
        z_copies.append(copy)
    copy = remote(m2.at[grp], m2.at[grp], c_send.at[0], c_recv.at[0], grp=other)
    copy.start()
    c_copies.append(copy)

    def couple(own, sources):
        spread = [jnp.broadcast_to(own[:, d : d + 1], (K, LANES)) for d in range(3)]
        total = jnp.zeros((R, K), jnp.float32)
        for first in range(0, len(sources), 4):
            highs, lows, parts = [], [], []
            for i in range(first, first + 4, 2):
                (v0, n0, odd0), (v1, n1, odd1) = sources[i], sources[i + 1]
                value = jnp.where(
                    low, jnp.concatenate([v0, swap(v0)], axis=0), jnp.concatenate([swap(v1), v1], axis=0)
                )
                n0 = jnp.where(odd0, swap(n0), n0)
                n1 = jnp.where(odd1, n1, swap(n1))
                place = jnp.where(low[:3], n0, n1) * 4.0
                d0, d1, d2 = (spread[d] - place[d : d + 1] for d in range(3))
                high, rest = split(lax.rsqrt(((1.0 + d0 * d0) + d1 * d1) + d2 * d2))
                highs.append(high)
                lows.append(rest)
                parts.append(value)
            value = jnp.concatenate(parts, axis=1)
            value_high, value_low = split(value)
            high, rest = jnp.concatenate(highs, axis=1), jnp.concatenate(lows, axis=1)
            both = dot(jnp.concatenate([value_high, value_low], axis=0), high, NT)
            total += both[:R] + both[R:] + dot(value_high, rest, NT)
        return total

    for copy in n_copies + second:
        copy.wait_recv()

    for step in range(1, n_grp // 2):
        z_copies[step - 1].wait_recv()
        block = m2.at[lax.rem(grp + n_grp - 2 * step, n_grp)]
        copy = remote(block, block, c_send.at[step], c_recv.at[step], grp=other)
        copy.start()
        c_copies.append(copy)

    def level_one(t, carry):
        sources = []
        for i in range(far1.shape[1]):
            s = lax.rem(far1[t, i], n_dev * boxes)
            home, box = lax.div(s, boxes), lax.rem(s, boxes)
            v = m1[lax.div(box, half_boxes), home * half_boxes + lax.rem(box, half_boxes)]
            both = near_nodes[home * (half_boxes // 2) + lax.div(box, 4)]
            n = jnp.where(lax.rem(lax.div(box, 2), 2) == 1, both[8:11], both[0:3])
            sources.append((v, n, lax.rem(box, 2) == 1))
        own = own_n[pl.ds(pl.multiple_of(t * K, K), K), :]
        acc[t, :, 0:HALF] = couple(own, sources)
        return carry

    lax.fori_loop(0, boxes, level_one, 0, unroll=2)

    for copy in c_copies:
        copy.wait_recv()

    def level_two(t, carry):
        target = box_parent[t]
        sources = []
        for i in range(far2.shape[0]):
            s = far2[i, target]
            v = m2[lax.div(s, n_dev), lax.rem(s, n_dev)]
            n = all_n2[lax.div(s, 2)][:3]
            sources.append((v, n, lax.rem(s, 2) == 1))
        own = own_n2[lax.rem(target, n_dev)]
        acc[t, :, HALF:LANES] = couple(own, sources)
        return carry

    lax.fori_loop(0, boxes, level_two, 0, unroll=2)

    for q in range(boxes // 2):
        rows = []
        for i in range(2):
            coarse = acc[2 * q + i]
            rows.append(jnp.where(low, swap(coarse), 0.0) if i == 0 else jnp.where(low, 0.0, coarse))
        moved = dot_split(jnp.concatenate(rows, axis=0), box_transfer[:, q * LANES : (q + 1) * LANES], NT)
        for i in range(2):
            g = acc[2 * q + i][:, :HALF] + moved[i * R : (i + 1) * R]
            g1[2 * q + i] = jnp.concatenate([g, g], axis=1)

    def descend(p, carry):
        top = g1[lax.rem(parent[2 * p], boxes)]
        bottom = g1[lax.rem(parent[2 * p + 1], boxes)]
        rows = jnp.concatenate([jnp.where(low, top, 0.0), jnp.where(low, 0.0, bottom)], axis=0)
        slab = transfer_v[:, pl.ds(pl.multiple_of(p * LANES, LANES), LANES)]
        high, rest = split(dot_split(rows, slab, NT))
        spread_g[p] = jnp.concatenate([high, rest, high], axis=1)
        return carry

    lax.fori_loop(0, leaves // 2, descend, 0, unroll=4)

    def evaluate(p, carry):
        left = spread_g[p]
        for i in range(2):
            at = pl.ds(pl.multiple_of((2 * p + i) * B, B), B)
            b_high, b_low = split(basis_v[:, at])
            far_out[:, at] = dot(left[i * R : (i + 1) * R], jnp.concatenate([b_high, b_high, b_low], axis=0), NN)
        return carry

    lax.fori_loop(0, leaves // 2, evaluate, 0, unroll=4)

    for copies in (n_copies, first, r_copies, d_copies, second, z_copies, c_copies):
        for copy in copies:
            copy.wait_send()
    for side in range(2):

        @pl.when(sends[side])
        def _():
            for copy in halo[side * per : (side + 1) * per]:
                copy.wait_send()

        @pl.when(sends[1 - side])
        def _():
            for copy in halo[side * per : (side + 1) * per]:
                copy.wait_recv()


def far_field(mesh_shape, count, parent, box_parent, far1, far2, points, rhs, basis, transfer, nodes, box_transfer, nodes2):
    n_grp, n_dev, n_x = mesh_shape
    n_y = n_dev // n_x
    boxes = box_parent.shape[0]
    leaves = count.shape[0]
    reach = REACH * B
    width = rhs.shape[1]
    vmem = pl.BlockSpec(memory_space=pltpu.VMEM)
    hbm = pl.BlockSpec(memory_space=pl.ANY)
    dma = pltpu.SemaphoreType.DMA
    small = (count, parent, box_parent, far1, far2)
    large = (nodes, box_transfer, nodes2, rhs, basis, transfer)
    return pl.pallas_call(
        functools.partial(far_kernel, mesh_shape),
        out_shape=(
            jax.ShapeDtypeStruct((2, R, reach), jnp.float32),
            jax.ShapeDtypeStruct((2, 3, reach), jnp.float32),
            jax.ShapeDtypeStruct((3, 1, leaves), jnp.int32),
            jax.ShapeDtypeStruct((R, width), jnp.float32),
        ),
        in_specs=[pl.BlockSpec(memory_space=pltpu.HBM)] * 13,
        out_specs=(hbm, hbm, hbm, vmem),
        scratch_shapes=[pltpu.SMEM(a.shape, jnp.int32) for a in small]
        + [pltpu.VMEM(a.shape, jnp.float32) for a in large]
        + [
            pltpu.VMEM((2, n_dev * (boxes // 2), 16, LANES), jnp.float32),
            pltpu.VMEM((n_dev * (boxes // 4), 16, LANES), jnp.float32),
            pltpu.VMEM((boxes, R, LANES), jnp.float32),
            pltpu.VMEM((boxes, R, LANES), jnp.float32),
            pltpu.VMEM((n_dev - 1, 16, LANES), jnp.float32),
            pltpu.VMEM((n_dev, 16, LANES), jnp.float32),
            pltpu.VMEM((n_grp, n_dev, 16, LANES), jnp.float32),
            pltpu.VMEM((boxes * K, 8), jnp.float32),
            pltpu.VMEM((n_dev, K, 8), jnp.float32),
            pltpu.VMEM((nodes2.shape[1] // LANES, 8, LANES), jnp.float32),
            pltpu.VMEM((leaves // 2, 2 * R, LANES), jnp.float32),
            pltpu.VMEM((leaves // 2, 2 * R, 3 * K), jnp.bfloat16),
            dma((11,)),
            dma((2, PIECES + 2)), dma((2, PIECES + 2)),
            dma((n_dev - 1,)), dma((n_dev - 1,)),
            dma((2, max(n_x, n_y) - 1)), dma((2, max(n_x, n_y) - 1)),
            dma((2, max(n_x, n_y) - 1, n_y)), dma((2, max(n_x, n_y) - 1, n_y)),
            dma((n_dev - 1,)), dma((n_dev - 1,)),
            dma((n_dev - 1,)), dma((n_dev - 1,)),
            dma((n_grp // 2 - 1,)), dma((n_grp // 2 - 1,)),
            dma((n_grp // 2,)), dma((n_grp // 2,)),
        ],
        compiler_params=pltpu.CompilerParams(collective_id=0, has_side_effects=True, vmem_limit_bytes=FAR_VMEM),
        cost_estimate=pl.CostEstimate(flops=10**9, bytes_accessed=10**7, transcendentals=10**6),
        name="far_field",
    )(count, parent, box_parent, far1, far2, points, rhs, basis, transfer, nodes, box_transfer, nodes2, count.reshape(1, 1, -1))


def local(
    mesh_shape,
    points,
    rhs,
    leaf_count,
    near_list,
    leaf_basis,
    leaf_transfer,
    leaf_parent,
    nodes1,
    box_transfer,
    box_parent,
    far1,
    nodes2,
    far2,
):
    leaves = leaf_count.shape[0]
    boxes = box_parent.shape[0]
    device = lax.axis_index("grp") * lax.axis_size("dev") + lax.axis_index("dev")
    halo_x, halo_p, halo_c, far = far_field(
        mesh_shape, leaf_count, leaf_parent, box_parent, far1, far2.T,
        points, rhs, leaf_basis, leaf_transfer, nodes1, box_transfer, nodes2,
    )
    place = jnp.stack([device * boxes, device * leaves - REACH])
    return near_field(place, halo_c, leaf_count, near_list.T, halo_x, halo_p, rhs, points, far)


def solution(mesh):
    placed = (
        P(None, ("grp", "dev")),
        P(None, ("grp", "dev")),
        P(("grp", "dev")),
        P(("grp", "dev"), None),
        P(None, ("grp", "dev")),
        P(None, ("grp", "dev")),
        P(("grp", "dev")),
        P(None, ("grp", "dev")),
        P(None, ("grp", "dev")),
        P(("grp", "dev")),
        P(("grp", "dev"), None),
        P(),
        P(),
    )
    mesh_shape = (mesh.shape["grp"], mesh.shape["dev"], 4)
    return jax.shard_map(
        functools.partial(local, mesh_shape),
        mesh=mesh, in_specs=placed, out_specs=P(None, ("grp", "dev")), check_vma=False
    )
```

```python
import functools

import jax
import jax.numpy as jnp
from jax import lax
from jax.experimental import pallas as pl
from jax.experimental.pallas import tpu as pltpu
from jax.sharding import PartitionSpec as P

B = 256
K = 64
R = 32
NEAR = 8
REACH = 32
LANES = 128
TILE = 32
SLOTS = 2
NEAR_VMEM = 62 * 1024 * 1024


def near_kernel(
    leaves, halo_c_h, own_c_h, rel_h, halo_x_h, halo_p_h, own_x_h, own_p_h, far_h, out,
    halo_c, own_c, rel, halo_x, halo_p, own_x, own_p, far, sems,
    xs, pb, ab, sums, lists, cnt, bases, turns, accs,
):
    pairs = [
        (halo_c_h, halo_c), (own_c_h, own_c), (rel_h, rel), (own_x_h, own_x), (own_p_h, own_p),
        (halo_x_h, halo_x), (halo_p_h, halo_p), (far_h, far),
    ]
    loads = [pltpu.make_async_copy(src, dst, sems.at[i]) for i, (src, dst) in enumerate(pairs)]
    for copy in loads:
        copy.start()
    halo = halo_x.shape[2] // B
    total = leaves + 2 * halo
    first_leaf = (lax.axis_index("grp") * lax.axis_size("dev") + lax.axis_index("dev")) * leaves - halo
    for copy in loads[:3]:
        copy.wait()
    for i in range(halo):
        cnt[i] = halo_c[0, 0, leaves - halo + i]
        cnt[halo + leaves + i] = halo_c[2, 0, i]
    for i in range(leaves):
        cnt[halo + i] = own_c[i]
    lane = lax.broadcasted_iota(jnp.int32, (R, B), 1)

    def load_source(src_x, src_p, first, i):
        at = pl.ds(pl.multiple_of(i * B, B), B)
        to = pl.ds(pl.multiple_of((first + i) * B, B), B)
        x = jnp.where(lane < cnt[first + i], src_x[:, at], 0.0)
        high = x.astype(jnp.bfloat16)
        xs[0:R, to] = high
        xs[R : 2 * R, to] = (x - high.astype(jnp.float32)).astype(jnp.bfloat16)
        scaled = src_p[:, at] * 4.0
        pb[0:3, to] = scaled

    def load_halo(i, carry):
        load_source(halo_x.at[0], halo_p.at[0], 0, i)
        load_source(halo_x.at[1], halo_p.at[1], halo + leaves, i)
        return carry

    tail = pl.ds(total * B, 2 * LANES)
    xs[:, tail] = jnp.zeros((2 * R, 2 * LANES), jnp.bfloat16)
    pb[:, tail] = jnp.zeros((8, 2 * LANES), jnp.float32)

    def spread(target, slot, half):
        at = pl.ds(pl.multiple_of((halo + target) * B + half * LANES, LANES), LANES)
        rows = pl.ds(pl.multiple_of(half * LANES, LANES), LANES)
        for d in range(3):
            ab[slot, d, rows, :] = jnp.broadcast_to(pb[d : d + 1, at], (LANES, LANES)).T

    def load_own(i, start):
        load_source(own_x, own_p, halo, i)
        at = start
        for n in range(NEAR):
            src = rel[n, i] - first_leaf
            lists[at] = 2 * src
            lists[at + 1] = 2 * src + 1
            at = at + 1 + (cnt[src] > LANES).astype(jnp.int32)
        lists[at] = 2 * total
        chunks = (at - start + 1) // 2
        at = start + 2 * chunks
        lists[at] = lists[at - 2]
        lists[at + 1] = lists[at - 1]
        bases[i] = start
        turns[i] = chunks
        return start + 4 * ((chunks + 1) // 2)

    for copy in loads[3:5]:
        copy.wait()
    end = lax.fori_loop(0, leaves, load_own, 0, unroll=4)
    for copy in loads[5:]:
        copy.wait()
    lax.fori_loop(0, halo, load_halo, 0, unroll=2)
    for half in range(B // LANES):
        spread(0, 0, half)
    for i in range(4):
        lists[end + i] = 2 * total

    def push(start):
        for unit in range(2):
            parts = []
            for half in range(2):
                at = lists[start + 2 * unit + half]
                parts.append(xs[:, pl.ds(pl.multiple_of(at * LANES, LANES), LANES)])
            w = jnp.concatenate(parts, axis=1)
            pltpu.matmul_push_rhs(jnp.concatenate([w] * 4, axis=0), 0, unit, transpose=True)

    def pop(slot, target):
        for t in range(B // TILE):
            both = pltpu.matmul_pop(accs[0][slot][t]) + pltpu.matmul_pop(accs[1][slot][t])
            sums[target, t * TILE : (t + 1) * TILE, :] = both[:, :LANES]

    def couple_step(slot, tiles, target, start, split_rows):
        cols = []
        for unit in range(1 if split_rows else 2):
            halves = []
            for half in range(2):
                at = lists[start + 2 * unit + half]
                at = pl.ds(pl.multiple_of(at * LANES, LANES), LANES)
                halves.append([pb[d : d + 1, at] for d in range(3)])
            cols.append(halves)
        fresh = [True, True]
        waiting = [[], []]
        for t in range(tiles):
            own = [ab[slot, d, t * TILE : (t + 1) * TILE, :] for d in range(3)]
            for unit in [t % 2] if split_rows else range(2):
                highs, lows = [], []
                for half in range(2):
                    col = cols[0 if split_rows else unit][half]
                    d0, d1, d2 = (own[d] - col[d] for d in range(3))
                    k = lax.rsqrt(((1.0 + d0 * d0) + d1 * d1) + d2 * d2)
                    high = k.astype(jnp.bfloat16)
                    highs.append(high)
                    lows.append((k - high.astype(jnp.float32)).astype(jnp.bfloat16))
                acc = accs[unit][slot][t]
                pltpu.matmul_acc_lhs(acc, jnp.concatenate(highs, axis=1), load_staged_rhs=0 if fresh[unit] else None)
                fresh[unit] = False
                for args in waiting[unit]:
                    pltpu.matmul_acc_lhs(*args)
                waiting[unit] = [(acc, jnp.concatenate(lows, axis=1))]
            if t == (1 if split_rows else 0):
                push(start + 4)
        for unit in range(2):
            for args in waiting[unit]:
                pltpu.matmul_acc_lhs(*args)

    def sweep(slot, tiles, target):
        start, count = bases[target], turns[target]

        def pair(i, carry):
            couple_step(slot, tiles, target, start + 4 * i, False)
            return carry

        for i in range(2):
            couple_step(slot, tiles, target, start + 4 * i, False)
            spread(jnp.minimum(target + 1, leaves - 1), 1 - slot, i)
        lax.fori_loop(2, lax.div(count, 2), pair, 0)

        @pl.when(lax.rem(count, 2) == 1)
        def _():
            couple_step(slot, tiles, target, start + 2 * (count - 1), True)

    for slot in range(SLOTS):
        pop(slot, leaves)
    push(0)

    def group(g, carry):
        for slot in range(SLOTS):
            target = SLOTS * g + slot
            kind = lax.div(cnt[halo + target] + (TILE - 1), TILE) - 2
            lax.switch(kind, [functools.partial(sweep, slot, tiles, target) for tiles in range(2, B // TILE + 1)])
            pop(1 - slot, jnp.where(target == 0, leaves, target - 1))
        return carry

    lax.fori_loop(0, leaves // SLOTS, group, 0)
    for unit in range(2):
        pltpu.matmul_acc_lhs(accs[unit][0][0], jnp.zeros((TILE, 2 * LANES), jnp.bfloat16), load_staged_rhs=0)
    pop(1, leaves - 1)
    pop(0, leaves)

    def finish(target, carry):
        parts = []
        for half in range(B // LANES):
            flipped = sums[target, half * LANES : (half + 1) * LANES, :].T
            parts.append(flipped[0:R] + flipped[R : 2 * R])
        at = pl.ds(pl.multiple_of(target * B, B), B)
        value = jnp.concatenate(parts, axis=1) + far[:, at]
        out[:, at] = jnp.where(lane < cnt[halo + target], value, 0.0)
        return carry

    lax.fori_loop(0, leaves, finish, 0, unroll=4)


def near_body(leaves, *refs):
    tiles = B // TILE
    specs = tuple(
        tuple(tuple(pltpu.ACC(unit)((TILE, 256), jnp.float32) for _ in range(tiles)) for _ in range(SLOTS))
        for unit in range(2)
    )
    pl.run_scoped(lambda accs: near_kernel(leaves, *refs, accs), specs)


def near_field(halo_c, own_c, rel, halo_x, halo_p, own_x, own_p, far):
    leaves = own_x.shape[1] // B
    extent = leaves + 2 * (halo_x.shape[2] // B)
    wide = extent * B + 2 * LANES
    small = (halo_c, own_c, rel)
    large = (halo_x, halo_p, own_x, own_p, far)
    return pl.pallas_call(
        functools.partial(near_body, leaves),
        out_shape=jax.ShapeDtypeStruct((R, leaves * B), jnp.float32),
        in_specs=[pl.BlockSpec(memory_space=pl.ANY)] * 8,
        out_specs=pl.BlockSpec(memory_space=pltpu.VMEM),
        scratch_shapes=[pltpu.SMEM(a.shape, jnp.int32) for a in small]
        + [pltpu.VMEM(a.shape, jnp.float32) for a in large]
        + [
            pltpu.SemaphoreType.DMA((8,)),
            pltpu.VMEM((2 * R, wide), jnp.bfloat16),
            pltpu.VMEM((8, wide), jnp.float32),
            pltpu.VMEM((SLOTS, 3, B, LANES), jnp.float32),
            pltpu.VMEM((leaves + 1, B, LANES), jnp.float32),
            pltpu.SMEM((leaves * 16 + 24,), jnp.int32),
            pltpu.SMEM((extent,), jnp.int32),
            pltpu.SMEM((leaves,), jnp.int32),
            pltpu.SMEM((leaves,), jnp.int32),
        ],
        compiler_params=pltpu.CompilerParams(vmem_limit_bytes=NEAR_VMEM),
        cost_estimate=pl.CostEstimate(flops=10**9, bytes_accessed=10**7, transcendentals=10**7),
        name="near_field",
    )(halo_c, own_c, rel, halo_x, halo_p, own_x, own_p, far)


MESH = pl.DeviceIdType.MESH
HALF = 64
PIECES = 8
FIRST_PIECES = 1
HALO_FIRST = 0
HALO_LAST = 2
ALONG_X = (True, False)
FAR_VMEM = 62 * 1024 * 1024
NT = (((1,), (1,)), ((), ()))
NN = (((1,), (0,)), ((), ()))


def split(x):
    high = x.astype(jnp.bfloat16)
    return high, (x - high.astype(jnp.float32)).astype(jnp.bfloat16)


def dot(a, b, dims):
    return lax.dot_general(a, b, dims, preferred_element_type=jnp.float32)


def dot_split(a, b, dims):
    a_high, a_low = split(a)
    b_high, b_low = split(b)
    rows = a.shape[0]
    both = dot(jnp.concatenate([a_high, a_low], axis=0), b_high, dims)
    return both[:rows] + both[rows:] + dot(a_high, b_low, dims)


def swap(x):
    return pltpu.roll(x, HALF, 1)


def fold(x):
    lane = lax.broadcasted_iota(jnp.int32, (16, LANES), 1)
    return jnp.where(lane < HALF, x[:16], x[16:])


def far_kernel(
    shape,
    count_h, parent_h, box_parent_h, far1_h, far2_h,
    points, rhs, basis, transfer, nodes_h, box_transfer_h, nodes2_h, counts,
    halo_x, halo_p, halo_c, far_out,
    count, parent, box_parent, far1, far2, nodes, box_transfer, nodes2,
    x_v, basis_v, transfer_v, m1, near_nodes, acc, g1, part, partial, m2, own_n, own_n2, all_n2, expanded, spread_g,
    load_sems, halo_send, halo_recv, n_send, n_recv, a_send, a_recv, b_send, b_recv,
    r_send, r_recv, d_send, d_recv, z_send, z_recv, c_send, c_recv,
):
    n_grp, n_dev, n_x = shape
    grp, dev = lax.axis_index("grp"), lax.axis_index("dev")
    n_y = n_dev // n_x
    my_y, my_x = dev // n_x, lax.rem(dev, n_x)
    leaves = parent.shape[0]
    boxes = box_parent.shape[0]
    reach = halo_x.shape[2]
    half_boxes = boxes // 2
    low = lax.broadcasted_iota(jnp.int32, (R, LANES), 1) < HALF

    pairs = [
        (nodes_h, nodes), (count_h, count), (parent_h, parent), (rhs, x_v), (basis, basis_v), (transfer, transfer_v),
        (box_parent_h, box_parent), (box_transfer_h, box_transfer), (far1_h, far1), (far2_h, far2), (nodes2_h, nodes2),
    ]
    loads = [pltpu.make_async_copy(src, dst, load_sems.at[i]) for i, (src, dst) in enumerate(pairs)]
    for copy in loads:
        copy.start()

    barrier = pltpu.get_barrier_semaphore()
    for step in range(1, n_dev):
        pl.semaphore_signal(barrier, inc=1, device_id={"dev": lax.rem(dev + step, n_dev)}, device_id_type=MESH)
    for to in [lax.rem(grp + 2 * step, n_grp) for step in range(1, n_grp // 2)] + [grp + 1 - 2 * lax.rem(grp, 2)]:
        pl.semaphore_signal(barrier, inc=1, device_id={"grp": to}, device_id_type=MESH)
    pl.semaphore_wait(barrier, n_dev - 1 + n_grp // 2)

    def remote(src, dst, send, recv, **place):
        return pltpu.make_async_remote_copy(
            src_ref=src, dst_ref=dst, send_sem=send, recv_sem=recv, device_id=place, device_id_type=MESH
        )

    width = x_v.shape[1]
    part_w = reach // PIECES
    halo = []
    for side in range(2):
        to = lax.rem(dev + (1 if side == 0 else n_dev - 1), n_dev)
        first = width - reach if side == 0 else 0
        for piece in range(PIECES):
            halo.append(
                remote(
                    rhs.at[:, pl.ds(first + piece * part_w, part_w)],
                    halo_x.at[side, :, pl.ds(piece * part_w, part_w)],
                    halo_send.at[side, piece],
                    halo_recv.at[side, piece],
                    dev=to,
                )
            )
        halo.append(
            remote(points.at[:, pl.ds(first, reach)], halo_p.at[side], halo_send.at[side, PIECES], halo_recv.at[side, PIECES], dev=to)
        )
        halo.append(
            remote(counts.at[0], halo_c.at[2 * side], halo_send.at[side, PIECES + 1], halo_recv.at[side, PIECES + 1], dev=to)
        )
    per = PIECES + 2
    sends = (dev < n_dev - 1, dev > 0)

    def start_halo(which):
        for side in range(2):

            @pl.when(sends[side])
            def _():
                for i in which:
                    halo[side * per + i].start()

    loads[0].wait()
    for q in range(half_boxes):
        near_nodes[dev * (half_boxes // 2) + q // 2, q % 2 * 8 : q % 2 * 8 + 3, :] = nodes[:, q * LANES : (q + 1) * LANES]
    own_nodes = near_nodes.at[pl.ds(dev * (half_boxes // 2), half_boxes // 2)]
    n_copies = []
    for step in range(1, n_dev):
        to = lax.rem(dev + step, n_dev)
        copy = remote(own_nodes, own_nodes, n_send.at[step - 1], n_recv.at[step - 1], dev=to)
        copy.start()
        n_copies.append(copy)
    start_halo([PIECES, PIECES + 1] + list(range(FIRST_PIECES)))

    acc[...] = jnp.zeros_like(acc)
    for copy in loads[1:]:
        copy.wait()
    slot = lax.broadcasted_iota(jnp.int32, (R, B), 1)

    def expand(p, carry):
        for i in range(2):
            c = 2 * p + i
            at = pl.ds(pl.multiple_of(c * B, B), B)
            x = jnp.where(slot < count[c], x_v[:, at], 0.0)
            x_high, x_low = split(x)
            b_high, b_low = split(basis_v[:, at])
            both = dot(jnp.concatenate([x_high, x_low], axis=0), jnp.concatenate([b_high, b_low], axis=0), NT)
            top, bottom = both[:R], both[R:]
            expanded[p, i * R : (i + 1) * R, :] = top + bottom + swap(top)
        return carry

    lax.fori_loop(0, leaves // 2, expand, 0, unroll=4)

    def lift(p, carry):
        slab = transfer_v[:, pl.ds(pl.multiple_of(p * LANES, LANES), LANES)]
        out = dot_split(expanded[p][:, :HALF], slab, NN)
        value = jnp.where(low, out[:R], out[R:])
        owner = jnp.where(low, parent[2 * p], parent[2 * p + 1]) - (grp * n_dev + dev) * boxes
        for b in range(boxes):
            acc[b] += jnp.where(owner == b, value, 0.0)
        return carry

    lax.fori_loop(0, leaves // 2, lift, 0, unroll=4)

    for b in range(boxes):
        full = acc[b] + swap(acc[b])
        acc[b] = full
        m1[b // half_boxes, dev * half_boxes + b % half_boxes] = fold(full)
    first, second = [], []

    def along(which, block, to, sem, copies):
        copy = remote(block, block, a_send.at[which, sem], a_recv.at[which, sem], dev=to)
        copy.start()
        copies.append(copy)

    mine = [m1.at[i, pl.ds(dev * half_boxes, half_boxes)] for i in range(2)]
    for which, along_x in enumerate(ALONG_X):
        for step in range(1, n_x if along_x else n_y):
            to = my_y * n_x + lax.rem(my_x + step, n_x) if along_x else lax.rem(my_y + step, n_y) * n_x + my_x
            along(which, mine[which], to, step - 1, first)

    sums = [jnp.zeros((16, LANES), jnp.float32) for _ in range(n_dev)]
    for q in range(boxes // 2):
        pair = jnp.concatenate([acc[2 * q], acc[2 * q + 1]], axis=0)[:, :HALF]
        out = dot_split(pair, box_transfer[:, q * LANES : (q + 1) * LANES], NN)
        for i in range(2):
            half = jnp.where(low == (i == 0), out[i * R : (i + 1) * R], 0.0)
            folded = fold(half + swap(half))
            owner = box_parent[2 * q + i] - grp * n_dev
            for p in range(n_dev):
                sums[p] += jnp.where(owner == p, folded, 0.0)
    for p in range(n_dev):
        partial[p] = sums[p]
    r_copies = []
    for step in range(1, n_dev):
        to = lax.rem(dev + step, n_dev)
        copy = remote(partial.at[to], part.at[step - 1], r_send.at[step - 1], r_recv.at[step - 1], dev=to)
        copy.start()
        r_copies.append(copy)
    start_halo(range(FIRST_PIECES, FIRST_PIECES + 1))

    for q in range(boxes // 2):
        own_n[q * LANES : (q + 1) * LANES, :] = (
            jnp.concatenate([nodes[:, q * LANES : (q + 1) * LANES], jnp.zeros((5, LANES), jnp.float32)], axis=0) * 4.0
        ).T
    for q in range(n_dev // 2):
        at = pl.ds(pl.multiple_of((grp * n_dev // 2 + q) * LANES, LANES), LANES)
        flipped = (jnp.concatenate([nodes2[:, at], jnp.zeros((5, LANES), jnp.float32)], axis=0) * 4.0).T
        own_n2[2 * q] = flipped[:K]
        own_n2[2 * q + 1] = flipped[K:]

    def spread_nodes(q, carry):
        all_n2[q, 0:3, :] = nodes2[:, pl.ds(pl.multiple_of(q * LANES, LANES), LANES)]
        return carry

    lax.fori_loop(0, nodes2.shape[1] // LANES, spread_nodes, 0, unroll=8)

    total = partial[dev]
    for step in range(1, n_dev):
        r_copies[step - 1].wait_recv()
        total += part[step - 1]
    m2[grp, dev] = total
    d_copies = []
    for step in range(1, n_dev):
        to = lax.rem(dev + step, n_dev)
        copy = remote(m2.at[grp, dev], m2.at[grp, dev], d_send.at[step - 1], d_recv.at[step - 1], dev=to)
        copy.start()
        d_copies.append(copy)
    for copy in first:
        copy.wait_recv()
    if HALO_FIRST:
        start_halo(range(FIRST_PIECES + 1, HALO_FIRST))
    for which, along_x in enumerate(ALONG_X):
        for step in range(1, n_y if along_x else n_x):
            if along_x:
                row = m1.at[which, pl.ds(my_y * n_x * half_boxes, n_x * half_boxes)]
                to = lax.rem(my_y + step, n_y) * n_x + my_x
                copy = remote(row, row, b_send.at[which, step - 1, 0], b_recv.at[which, step - 1, 0], dev=to)
                copy.start()
                second.append(copy)
            else:
                for y in range(n_y):
                    piece = m1.at[which, pl.ds((y * n_x + my_x) * half_boxes, half_boxes)]
                    to = my_y * n_x + lax.rem(my_x + step, n_x)
                    copy = remote(piece, piece, b_send.at[which, step - 1, y], b_recv.at[which, step - 1, y], dev=to)
                    copy.start()
                    second.append(copy)
    start_halo(range(max(FIRST_PIECES + 1, HALO_FIRST), HALO_LAST))
    for copy in d_copies:
        copy.wait_recv()
    other = grp + 1 - 2 * lax.rem(grp, 2)
    z_copies, c_copies = [], []
    for step in range(1, n_grp // 2):
        to = lax.rem(grp + 2 * step, n_grp)
        copy = remote(m2.at[grp], m2.at[grp], z_send.at[step - 1], z_recv.at[step - 1], grp=to)
        copy.start()
        z_copies.append(copy)
    copy = remote(m2.at[grp], m2.at[grp], c_send.at[0], c_recv.at[0], grp=other)
    copy.start()
    c_copies.append(copy)

    def couple(own, sources):
        spread = [jnp.broadcast_to(own[:, d : d + 1], (K, LANES)) for d in range(3)]
        total = jnp.zeros((R, K), jnp.float32)
        for first in range(0, len(sources), 4):
            highs, lows, parts = [], [], []
            for i in range(first, first + 4, 2):
                (v0, n0, odd0), (v1, n1, odd1) = sources[i], sources[i + 1]
                value = jnp.where(
                    low, jnp.concatenate([v0, swap(v0)], axis=0), jnp.concatenate([swap(v1), v1], axis=0)
                )
                n0 = jnp.where(odd0, swap(n0), n0)
                n1 = jnp.where(odd1, n1, swap(n1))
                place = jnp.where(low[:3], n0, n1) * 4.0
                d0, d1, d2 = (spread[d] - place[d : d + 1] for d in range(3))
                high, rest = split(lax.rsqrt(((1.0 + d0 * d0) + d1 * d1) + d2 * d2))
                highs.append(high)
                lows.append(rest)
                parts.append(value)
            value = jnp.concatenate(parts, axis=1)
            value_high, value_low = split(value)
            high, rest = jnp.concatenate(highs, axis=1), jnp.concatenate(lows, axis=1)
            both = dot(jnp.concatenate([value_high, value_low], axis=0), high, NT)
            total += both[:R] + both[R:] + dot(value_high, rest, NT)
        return total

    for copy in n_copies + second:
        copy.wait_recv()
    start_halo(range(HALO_LAST, PIECES))

    for step in range(1, n_grp // 2):
        z_copies[step - 1].wait_recv()
        block = m2.at[lax.rem(grp + n_grp - 2 * step, n_grp)]
        copy = remote(block, block, c_send.at[step], c_recv.at[step], grp=other)
        copy.start()
        c_copies.append(copy)

    def level_one(t, carry):
        sources = []
        for i in range(far1.shape[1]):
            s = lax.rem(far1[t, i], n_dev * boxes)
            home, box = lax.div(s, boxes), lax.rem(s, boxes)
            v = m1[lax.div(box, half_boxes), home * half_boxes + lax.rem(box, half_boxes)]
            both = near_nodes[home * (half_boxes // 2) + lax.div(box, 4)]
            n = jnp.where(lax.rem(lax.div(box, 2), 2) == 1, both[8:11], both[0:3])
            sources.append((v, n, lax.rem(box, 2) == 1))
        own = own_n[pl.ds(pl.multiple_of(t * K, K), K), :]
        acc[t, :, 0:HALF] = couple(own, sources)
        return carry

    lax.fori_loop(0, boxes, level_one, 0, unroll=2)

    for copy in c_copies:
        copy.wait_recv()

    def level_two(t, carry):
        target = box_parent[t]
        sources = []
        for i in range(far2.shape[0]):
            s = far2[i, target]
            v = m2[lax.div(s, n_dev), lax.rem(s, n_dev)]
            n = all_n2[lax.div(s, 2)][:3]
            sources.append((v, n, lax.rem(s, 2) == 1))
        own = own_n2[lax.rem(target, n_dev)]
        acc[t, :, HALF:LANES] = couple(own, sources)
        return carry

    lax.fori_loop(0, boxes, level_two, 0, unroll=2)

    for q in range(boxes // 2):
        rows = []
        for i in range(2):
            coarse = acc[2 * q + i]
            rows.append(jnp.where(low, swap(coarse), 0.0) if i == 0 else jnp.where(low, 0.0, coarse))
        moved = dot_split(jnp.concatenate(rows, axis=0), box_transfer[:, q * LANES : (q + 1) * LANES], NT)
        for i in range(2):
            g = acc[2 * q + i][:, :HALF] + moved[i * R : (i + 1) * R]
            g1[2 * q + i] = jnp.concatenate([g, g], axis=1)

    def descend(p, carry):
        top = g1[lax.rem(parent[2 * p], boxes)]
        bottom = g1[lax.rem(parent[2 * p + 1], boxes)]
        rows = jnp.concatenate([jnp.where(low, top, 0.0), jnp.where(low, 0.0, bottom)], axis=0)
        slab = transfer_v[:, pl.ds(pl.multiple_of(p * LANES, LANES), LANES)]
        high, rest = split(dot_split(rows, slab, NT))
        spread_g[p] = jnp.concatenate([high, rest, high], axis=1)
        return carry

    lax.fori_loop(0, leaves // 2, descend, 0, unroll=4)

    def evaluate(p, carry):
        left = spread_g[p]
        for i in range(2):
            at = pl.ds(pl.multiple_of((2 * p + i) * B, B), B)
            b_high, b_low = split(basis_v[:, at])
            far_out[:, at] = dot(left[i * R : (i + 1) * R], jnp.concatenate([b_high, b_high, b_low], axis=0), NN)
        return carry

    lax.fori_loop(0, leaves // 2, evaluate, 0, unroll=4)

    for copies in (n_copies, first, r_copies, d_copies, second, z_copies, c_copies):
        for copy in copies:
            copy.wait_send()
    for side in range(2):

        @pl.when(sends[side])
        def _():
            for copy in halo[side * per : (side + 1) * per]:
                copy.wait_send()

        @pl.when(sends[1 - side])
        def _():
            for copy in halo[side * per : (side + 1) * per]:
                copy.wait_recv()


def far_field(mesh_shape, count, parent, box_parent, far1, far2, points, rhs, basis, transfer, nodes, box_transfer, nodes2):
    n_grp, n_dev, n_x = mesh_shape
    n_y = n_dev // n_x
    boxes = box_parent.shape[0]
    leaves = count.shape[0]
    reach = REACH * B
    width = rhs.shape[1]
    vmem = pl.BlockSpec(memory_space=pltpu.VMEM)
    hbm = pl.BlockSpec(memory_space=pl.ANY)
    dma = pltpu.SemaphoreType.DMA
    small = (count, parent, box_parent, far1, far2)
    large = (nodes, box_transfer, nodes2, rhs, basis, transfer)
    return pl.pallas_call(
        functools.partial(far_kernel, mesh_shape),
        out_shape=(
            jax.ShapeDtypeStruct((2, R, reach), jnp.float32),
            jax.ShapeDtypeStruct((2, 3, reach), jnp.float32),
            jax.ShapeDtypeStruct((3, 1, leaves), jnp.int32),
            jax.ShapeDtypeStruct((R, width), jnp.float32),
        ),
        in_specs=[pl.BlockSpec(memory_space=pltpu.HBM)] * 13,
        out_specs=(hbm, hbm, hbm, vmem),
        scratch_shapes=[pltpu.SMEM(a.shape, jnp.int32) for a in small]
        + [pltpu.VMEM(a.shape, jnp.float32) for a in large]
        + [
            pltpu.VMEM((2, n_dev * (boxes // 2), 16, LANES), jnp.float32),
            pltpu.VMEM((n_dev * (boxes // 4), 16, LANES), jnp.float32),
            pltpu.VMEM((boxes, R, LANES), jnp.float32),
            pltpu.VMEM((boxes, R, LANES), jnp.float32),
            pltpu.VMEM((n_dev - 1, 16, LANES), jnp.float32),
            pltpu.VMEM((n_dev, 16, LANES), jnp.float32),
            pltpu.VMEM((n_grp, n_dev, 16, LANES), jnp.float32),
            pltpu.VMEM((boxes * K, 8), jnp.float32),
            pltpu.VMEM((n_dev, K, 8), jnp.float32),
            pltpu.VMEM((nodes2.shape[1] // LANES, 8, LANES), jnp.float32),
            pltpu.VMEM((leaves // 2, 2 * R, LANES), jnp.float32),
            pltpu.VMEM((leaves // 2, 2 * R, 3 * K), jnp.bfloat16),
            dma((11,)),
            dma((2, PIECES + 2)), dma((2, PIECES + 2)),
            dma((n_dev - 1,)), dma((n_dev - 1,)),
            dma((2, max(n_x, n_y) - 1)), dma((2, max(n_x, n_y) - 1)),
            dma((2, max(n_x, n_y) - 1, n_y)), dma((2, max(n_x, n_y) - 1, n_y)),
            dma((n_dev - 1,)), dma((n_dev - 1,)),
            dma((n_dev - 1,)), dma((n_dev - 1,)),
            dma((n_grp // 2 - 1,)), dma((n_grp // 2 - 1,)),
            dma((n_grp // 2,)), dma((n_grp // 2,)),
        ],
        compiler_params=pltpu.CompilerParams(collective_id=0, has_side_effects=True, vmem_limit_bytes=FAR_VMEM),
        cost_estimate=pl.CostEstimate(flops=10**9, bytes_accessed=10**7, transcendentals=10**6),
        name="far_field",
    )(count, parent, box_parent, far1, far2, points, rhs, basis, transfer, nodes, box_transfer, nodes2, count.reshape(1, 1, -1))


def local(
    mesh_shape,
    points,
    rhs,
    leaf_count,
    near_list,
    leaf_basis,
    leaf_transfer,
    leaf_parent,
    nodes1,
    box_transfer,
    box_parent,
    far1,
    nodes2,
    far2,
):
    halo_x, halo_p, halo_c, far = far_field(
        mesh_shape, leaf_count, leaf_parent, box_parent, far1, far2.T,
        points, rhs, leaf_basis, leaf_transfer, nodes1, box_transfer, nodes2,
    )
    return near_field(halo_c, leaf_count, near_list.T, halo_x, halo_p, rhs, points, far)


def solution(mesh):
    placed = (
        P(None, ("grp", "dev")),
        P(None, ("grp", "dev")),
        P(("grp", "dev")),
        P(("grp", "dev"), None),
        P(None, ("grp", "dev")),
        P(None, ("grp", "dev")),
        P(("grp", "dev")),
        P(None, ("grp", "dev")),
        P(None, ("grp", "dev")),
        P(("grp", "dev")),
        P(("grp", "dev"), None),
        P(),
        P(),
    )
    mesh_shape = (mesh.shape["grp"], mesh.shape["dev"], 4)
    return jax.shard_map(
        functools.partial(local, mesh_shape),
        mesh=mesh, in_specs=placed, out_specs=P(None, ("grp", "dev")), check_vma=False
    )
```

```python
import functools

import jax
import jax.numpy as jnp
from jax import lax
from jax.experimental import pallas as pl
from jax.experimental.pallas import tpu as pltpu
from jax.sharding import PartitionSpec as P

B = 256
K = 64
R = 32
NEAR = 8
REACH = 32
LANES = 128
TILE = 32
SLOTS = 2
NEAR_VMEM = 62 * 1024 * 1024


def near_kernel(
    leaves, halo_c_h, own_c_h, rel_h, halo_x_h, halo_p_h, own_x_h, own_p_h, far_h, out,
    halo_c, own_c, rel, halo_x, halo_p, own_x, own_p, far, sems,
    xs, pb, ab, sums, lists, cnt, bases, turns, accs,
):
    pairs = [
        (halo_c_h, halo_c), (own_c_h, own_c), (rel_h, rel), (own_x_h, own_x), (own_p_h, own_p),
        (halo_x_h, halo_x), (halo_p_h, halo_p), (far_h, far),
    ]
    loads = [pltpu.make_async_copy(src, dst, sems.at[i]) for i, (src, dst) in enumerate(pairs)]
    for copy in loads:
        copy.start()
    halo = halo_x.shape[2] // B
    total = leaves + 2 * halo
    first_leaf = (lax.axis_index("grp") * lax.axis_size("dev") + lax.axis_index("dev")) * leaves - halo
    for copy in loads[:3]:
        copy.wait()
    for i in range(halo):
        cnt[i] = halo_c[0, 0, leaves - halo + i]
        cnt[halo + leaves + i] = halo_c[2, 0, i]
    for i in range(leaves):
        cnt[halo + i] = own_c[i]
    lane = lax.broadcasted_iota(jnp.int32, (R, B), 1)

    def load_source(src_x, src_p, first, i):
        at = pl.ds(pl.multiple_of(i * B, B), B)
        to = pl.ds(pl.multiple_of((first + i) * B, B), B)
        x = jnp.where(lane < cnt[first + i], src_x[:, at], 0.0)
        high = x.astype(jnp.bfloat16)
        xs[0:R, to] = high
        xs[R : 2 * R, to] = (x - high.astype(jnp.float32)).astype(jnp.bfloat16)
        scaled = src_p[:, at] * 4.0
        pb[0:3, to] = scaled

    def load_halo(i, carry):
        load_source(halo_x.at[0], halo_p.at[0], 0, i)
        load_source(halo_x.at[1], halo_p.at[1], halo + leaves, i)
        return carry

    tail = pl.ds(total * B, 2 * LANES)
    xs[:, tail] = jnp.zeros((2 * R, 2 * LANES), jnp.bfloat16)
    pb[:, tail] = jnp.zeros((8, 2 * LANES), jnp.float32)

    def spread(target, slot, half):
        at = pl.ds(pl.multiple_of((halo + target) * B + half * LANES, LANES), LANES)
        rows = pl.ds(pl.multiple_of(half * LANES, LANES), LANES)
        for d in range(3):
            ab[slot, d, rows, :] = jnp.broadcast_to(pb[d : d + 1, at], (LANES, LANES)).T

    def load_own(i, carry):
        load_source(own_x, own_p, halo, i)
        return carry

    def list_blocks(target):
        start = bases[target]
        at = start
        for n in range(NEAR):
            src = rel[n, jnp.minimum(target, leaves - 1)] - first_leaf
            lists[at] = 2 * src
            lists[at + 1] = 2 * src + 1
            at = at + 1 + (cnt[src] > LANES).astype(jnp.int32)
        lists[at] = 2 * total
        chunks = lax.div(at - start + 1, 2)
        at = start + 2 * chunks
        lists[at] = lists[at - 2]
        lists[at + 1] = lists[at - 1]
        turns[target] = chunks
        bases[target + 1] = start + 4 * lax.div(chunks + 1, 2)

    for copy in loads[3:5]:
        copy.wait()
    lax.fori_loop(0, leaves, load_own, 0, unroll=4)
    for copy in loads[5:]:
        copy.wait()
    lax.fori_loop(0, halo, load_halo, 0, unroll=2)
    for half in range(B // LANES):
        spread(0, 0, half)
    bases[0] = 0
    list_blocks(0)

    def push(start):
        for unit in range(2):
            parts = []
            for half in range(2):
                at = lists[start + 2 * unit + half]
                parts.append(xs[:, pl.ds(pl.multiple_of(at * LANES, LANES), LANES)])
            w = jnp.concatenate(parts, axis=1)
            pltpu.matmul_push_rhs(jnp.concatenate([w] * 4, axis=0), 0, unit, transpose=True)

    def pop(slot, target):
        for t in range(B // TILE):
            both = pltpu.matmul_pop(accs[0][slot][t]) + pltpu.matmul_pop(accs[1][slot][t])
            sums[target, t * TILE : (t + 1) * TILE, :] = both[:, :LANES]

    def couple_step(slot, tiles, target, start, split_rows):
        cols = []
        for unit in range(1 if split_rows else 2):
            halves = []
            for half in range(2):
                at = lists[start + 2 * unit + half]
                at = pl.ds(pl.multiple_of(at * LANES, LANES), LANES)
                halves.append([pb[d : d + 1, at] for d in range(3)])
            cols.append(halves)
        fresh = [True, True]
        waiting = [[], []]
        for t in range(tiles):
            own = [ab[slot, d, t * TILE : (t + 1) * TILE, :] for d in range(3)]
            for unit in [t % 2] if split_rows else range(2):
                highs, lows = [], []
                for half in range(2):
                    col = cols[0 if split_rows else unit][half]
                    d0, d1, d2 = (own[d] - col[d] for d in range(3))
                    k = lax.rsqrt(((1.0 + d0 * d0) + d1 * d1) + d2 * d2)
                    highs.append(k)
                    lows.append(k - k.astype(jnp.bfloat16).astype(jnp.float32))
                acc = accs[unit][slot][t]
                pltpu.matmul_acc_lhs(acc, jnp.concatenate(highs, axis=1), load_staged_rhs=0 if fresh[unit] else None)
                fresh[unit] = False
                for args in waiting[unit]:
                    pltpu.matmul_acc_lhs(*args)
                waiting[unit] = [(acc, jnp.concatenate(lows, axis=1))]
            if t == (1 if split_rows else 0):
                push(start + 4)
        for unit in range(2):
            for args in waiting[unit]:
                pltpu.matmul_acc_lhs(*args)

    def sweep(slot, tiles, target):
        start, count = bases[target], turns[target]

        def pair(i, carry):
            couple_step(slot, tiles, target, start + 4 * i, False)
            return carry

        list_blocks(target + 1)
        for i in range(2):
            couple_step(slot, tiles, target, start + 4 * i, False)
            spread(jnp.minimum(target + 1, leaves - 1), 1 - slot, i)
        lax.fori_loop(2, lax.div(count, 2), pair, 0)

        @pl.when(lax.rem(count, 2) == 1)
        def _():
            couple_step(slot, tiles, target, start + 2 * (count - 1), True)

    for slot in range(SLOTS):
        pop(slot, leaves)
    push(0)

    def group(g, carry):
        for slot in range(SLOTS):
            target = SLOTS * g + slot
            kind = lax.div(cnt[halo + target] + (TILE - 1), TILE) - 2
            lax.switch(kind, [functools.partial(sweep, slot, tiles, target) for tiles in range(2, B // TILE + 1)])
            pop(1 - slot, jnp.where(target == 0, leaves, target - 1))
        return carry

    lax.fori_loop(0, leaves // SLOTS, group, 0)
    for unit in range(2):
        pltpu.matmul_acc_lhs(accs[unit][0][0], jnp.zeros((TILE, 2 * LANES), jnp.bfloat16), load_staged_rhs=0)
    pop(1, leaves - 1)
    pop(0, leaves)

    def finish(target, carry):
        parts = []
        for half in range(B // LANES):
            flipped = sums[target, half * LANES : (half + 1) * LANES, :].T
            parts.append(flipped[0:R] + flipped[R : 2 * R])
        at = pl.ds(pl.multiple_of(target * B, B), B)
        value = jnp.concatenate(parts, axis=1) + far[:, at]
        out[:, at] = jnp.where(lane < cnt[halo + target], value, 0.0)
        return carry

    lax.fori_loop(0, leaves, finish, 0, unroll=4)


def near_body(leaves, *refs):
    tiles = B // TILE
    specs = tuple(
        tuple(tuple(pltpu.ACC(unit)((TILE, 256), jnp.float32) for _ in range(tiles)) for _ in range(SLOTS))
        for unit in range(2)
    )
    pl.run_scoped(lambda accs: near_kernel(leaves, *refs, accs), specs)


def near_field(halo_c, own_c, rel, halo_x, halo_p, own_x, own_p, far):
    leaves = own_x.shape[1] // B
    extent = leaves + 2 * (halo_x.shape[2] // B)
    wide = extent * B + 2 * LANES
    small = (halo_c, own_c, rel)
    large = (halo_x, halo_p, own_x, own_p, far)
    return pl.pallas_call(
        functools.partial(near_body, leaves),
        out_shape=jax.ShapeDtypeStruct((R, leaves * B), jnp.float32),
        in_specs=[pl.BlockSpec(memory_space=pl.ANY)] * 8,
        out_specs=pl.BlockSpec(memory_space=pltpu.VMEM),
        scratch_shapes=[pltpu.SMEM(a.shape, jnp.int32) for a in small]
        + [pltpu.VMEM(a.shape, jnp.float32) for a in large]
        + [
            pltpu.SemaphoreType.DMA((8,)),
            pltpu.VMEM((2 * R, wide), jnp.bfloat16),
            pltpu.VMEM((8, wide), jnp.float32),
            pltpu.VMEM((SLOTS, 3, B, LANES), jnp.float32),
            pltpu.VMEM((leaves + 1, B, LANES), jnp.float32),
            pltpu.SMEM((leaves * 16 + 40,), jnp.int32),
            pltpu.SMEM((extent,), jnp.int32),
            pltpu.SMEM((leaves + 2,), jnp.int32),
            pltpu.SMEM((leaves + 2,), jnp.int32),
        ],
        compiler_params=pltpu.CompilerParams(vmem_limit_bytes=NEAR_VMEM),
        cost_estimate=pl.CostEstimate(flops=10**9, bytes_accessed=10**7, transcendentals=10**7),
        name="near_field",
    )(halo_c, own_c, rel, halo_x, halo_p, own_x, own_p, far)


MESH = pl.DeviceIdType.MESH
HALF = 64
PIECES = 8
FIRST_PIECES = 1
HALO_FIRST = 0
HALO_LAST = 2
ALONG_X = (True, False)
FAR_VMEM = 62 * 1024 * 1024
NT = (((1,), (1,)), ((), ()))
NN = (((1,), (0,)), ((), ()))


def split(x):
    high = x.astype(jnp.bfloat16)
    return high, (x - high.astype(jnp.float32)).astype(jnp.bfloat16)


def dot(a, b, dims):
    return lax.dot_general(a, b, dims, preferred_element_type=jnp.float32)


def dot_split(a, b, dims):
    a_high, a_low = split(a)
    b_high, b_low = split(b)
    rows = a.shape[0]
    both = dot(jnp.concatenate([a_high, a_low], axis=0), b_high, dims)
    return both[:rows] + both[rows:] + dot(a_high, b_low, dims)


def swap(x):
    return pltpu.roll(x, HALF, 1)


def fold(x):
    lane = lax.broadcasted_iota(jnp.int32, (16, LANES), 1)
    return jnp.where(lane < HALF, x[:16], x[16:])


def far_kernel(
    shape,
    count_h, parent_h, box_parent_h, far1_h, far2_h,
    points, rhs, basis, transfer, nodes_h, box_transfer_h, nodes2_h, counts,
    halo_x, halo_p, halo_c, far_out,
    count, parent, box_parent, far1, far2, nodes, box_transfer, nodes2,
    x_v, basis_v, transfer_v, m1, near_nodes, acc, g1, part, partial, m2, own_n, own_n2, all_n2, expanded, spread_g,
    load_sems, halo_send, halo_recv, n_send, n_recv, a_send, a_recv, b_send, b_recv,
    r_send, r_recv, d_send, d_recv, z_send, z_recv, c_send, c_recv,
):
    n_grp, n_dev, n_x = shape
    grp, dev = lax.axis_index("grp"), lax.axis_index("dev")
    n_y = n_dev // n_x
    my_y, my_x = dev // n_x, lax.rem(dev, n_x)
    leaves = parent.shape[0]
    boxes = box_parent.shape[0]
    reach = halo_x.shape[2]
    half_boxes = boxes // 2
    low = lax.broadcasted_iota(jnp.int32, (R, LANES), 1) < HALF

    pairs = [
        (nodes_h, nodes), (count_h, count), (parent_h, parent), (rhs, x_v), (basis, basis_v), (transfer, transfer_v),
        (box_parent_h, box_parent), (box_transfer_h, box_transfer), (far1_h, far1), (far2_h, far2), (nodes2_h, nodes2),
    ]
    loads = [pltpu.make_async_copy(src, dst, load_sems.at[i]) for i, (src, dst) in enumerate(pairs)]
    for copy in loads:
        copy.start()

    barrier = pltpu.get_barrier_semaphore()
    for step in range(1, n_dev):
        pl.semaphore_signal(barrier, inc=1, device_id={"dev": lax.rem(dev + step, n_dev)}, device_id_type=MESH)
    for to in [lax.rem(grp + 2 * step, n_grp) for step in range(1, n_grp // 2)] + [grp + 1 - 2 * lax.rem(grp, 2)]:
        pl.semaphore_signal(barrier, inc=1, device_id={"grp": to}, device_id_type=MESH)
    pl.semaphore_wait(barrier, n_dev - 1 + n_grp // 2)

    def remote(src, dst, send, recv, **place):
        return pltpu.make_async_remote_copy(
            src_ref=src, dst_ref=dst, send_sem=send, recv_sem=recv, device_id=place, device_id_type=MESH
        )

    width = x_v.shape[1]
    part_w = reach // PIECES
    halo = []
    for side in range(2):
        to = lax.rem(dev + (1 if side == 0 else n_dev - 1), n_dev)
        first = width - reach if side == 0 else 0
        for piece in range(PIECES):
            halo.append(
                remote(
                    rhs.at[:, pl.ds(first + piece * part_w, part_w)],
                    halo_x.at[side, :, pl.ds(piece * part_w, part_w)],
                    halo_send.at[side, piece],
                    halo_recv.at[side, piece],
                    dev=to,
                )
            )
        halo.append(
            remote(points.at[:, pl.ds(first, reach)], halo_p.at[side], halo_send.at[side, PIECES], halo_recv.at[side, PIECES], dev=to)
        )
        halo.append(
            remote(counts.at[0], halo_c.at[2 * side], halo_send.at[side, PIECES + 1], halo_recv.at[side, PIECES + 1], dev=to)
        )
    per = PIECES + 2
    sends = (dev < n_dev - 1, dev > 0)

    def start_halo(which):
        for side in range(2):

            @pl.when(sends[side])
            def _():
                for i in which:
                    halo[side * per + i].start()

    loads[0].wait()
    for q in range(half_boxes):
        near_nodes[dev * (half_boxes // 2) + q // 2, q % 2 * 8 : q % 2 * 8 + 3, :] = nodes[:, q * LANES : (q + 1) * LANES]
    own_nodes = near_nodes.at[pl.ds(dev * (half_boxes // 2), half_boxes // 2)]
    n_copies = []
    for step in range(1, n_dev):
        to = lax.rem(dev + step, n_dev)
        copy = remote(own_nodes, own_nodes, n_send.at[step - 1], n_recv.at[step - 1], dev=to)
        copy.start()
        n_copies.append(copy)
    start_halo([PIECES, PIECES + 1] + list(range(FIRST_PIECES)))

    acc[...] = jnp.zeros_like(acc)
    for copy in loads[1:]:
        copy.wait()
    slot = lax.broadcasted_iota(jnp.int32, (R, B), 1)

    def expand(p, carry):
        for i in range(2):
            c = 2 * p + i
            at = pl.ds(pl.multiple_of(c * B, B), B)
            x = jnp.where(slot < count[c], x_v[:, at], 0.0)
            x_high, x_low = split(x)
            b_high, b_low = split(basis_v[:, at])
            both = dot(jnp.concatenate([x_high, x_low], axis=0), jnp.concatenate([b_high, b_low], axis=0), NT)
            top, bottom = both[:R], both[R:]
            expanded[p, i * R : (i + 1) * R, :] = top + bottom + swap(top)
        return carry

    lax.fori_loop(0, leaves // 2, expand, 0, unroll=4)

    def lift(p, carry):
        slab = transfer_v[:, pl.ds(pl.multiple_of(p * LANES, LANES), LANES)]
        out = dot_split(expanded[p][:, :HALF], slab, NN)
        value = jnp.where(low, out[:R], out[R:])
        owner = jnp.where(low, parent[2 * p], parent[2 * p + 1]) - (grp * n_dev + dev) * boxes
        for b in range(boxes):
            acc[b] += jnp.where(owner == b, value, 0.0)
        return carry

    lax.fori_loop(0, leaves // 2, lift, 0, unroll=4)

    for b in range(boxes):
        full = acc[b] + swap(acc[b])
        acc[b] = full
        m1[b // half_boxes, dev * half_boxes + b % half_boxes] = fold(full)
    first, second = [], []

    def along(which, block, to, sem, copies):
        copy = remote(block, block, a_send.at[which, sem], a_recv.at[which, sem], dev=to)
        copy.start()
        copies.append(copy)

    mine = [m1.at[i, pl.ds(dev * half_boxes, half_boxes)] for i in range(2)]
    for which, along_x in enumerate(ALONG_X):
        for step in range(1, n_x if along_x else n_y):
            to = my_y * n_x + lax.rem(my_x + step, n_x) if along_x else lax.rem(my_y + step, n_y) * n_x + my_x
            along(which, mine[which], to, step - 1, first)

    sums = [jnp.zeros((16, LANES), jnp.float32) for _ in range(n_dev)]
    for q in range(boxes // 2):
        pair = jnp.concatenate([acc[2 * q], acc[2 * q + 1]], axis=0)[:, :HALF]
        out = dot_split(pair, box_transfer[:, q * LANES : (q + 1) * LANES], NN)
        for i in range(2):
            half = jnp.where(low == (i == 0), out[i * R : (i + 1) * R], 0.0)
            folded = fold(half + swap(half))
            owner = box_parent[2 * q + i] - grp * n_dev
            for p in range(n_dev):
                sums[p] += jnp.where(owner == p, folded, 0.0)
    for p in range(n_dev):
        partial[p] = sums[p]
    r_copies = []
    for step in range(1, n_dev):
        to = lax.rem(dev + step, n_dev)
        copy = remote(partial.at[to], part.at[step - 1], r_send.at[step - 1], r_recv.at[step - 1], dev=to)
        copy.start()
        r_copies.append(copy)
    start_halo(range(FIRST_PIECES, FIRST_PIECES + 1))

    for q in range(boxes // 2):
        own_n[q * LANES : (q + 1) * LANES, :] = (
            jnp.concatenate([nodes[:, q * LANES : (q + 1) * LANES], jnp.zeros((5, LANES), jnp.float32)], axis=0) * 4.0
        ).T
    for q in range(n_dev // 2):
        at = pl.ds(pl.multiple_of((grp * n_dev // 2 + q) * LANES, LANES), LANES)
        flipped = (jnp.concatenate([nodes2[:, at], jnp.zeros((5, LANES), jnp.float32)], axis=0) * 4.0).T
        own_n2[2 * q] = flipped[:K]
        own_n2[2 * q + 1] = flipped[K:]

    def spread_nodes(q, carry):
        all_n2[q, 0:3, :] = nodes2[:, pl.ds(pl.multiple_of(q * LANES, LANES), LANES)]
        return carry

    lax.fori_loop(0, nodes2.shape[1] // LANES, spread_nodes, 0, unroll=8)

    total = partial[dev]
    for step in range(1, n_dev):
        r_copies[step - 1].wait_recv()
        total += part[step - 1]
    m2[grp, dev] = total
    d_copies = []
    for step in range(1, n_dev):
        to = lax.rem(dev + step, n_dev)
        copy = remote(m2.at[grp, dev], m2.at[grp, dev], d_send.at[step - 1], d_recv.at[step - 1], dev=to)
        copy.start()
        d_copies.append(copy)
    for copy in first:
        copy.wait_recv()
    if HALO_FIRST:
        start_halo(range(FIRST_PIECES + 1, HALO_FIRST))
    for which, along_x in enumerate(ALONG_X):
        for step in range(1, n_y if along_x else n_x):
            if along_x:
                row = m1.at[which, pl.ds(my_y * n_x * half_boxes, n_x * half_boxes)]
                to = lax.rem(my_y + step, n_y) * n_x + my_x
                copy = remote(row, row, b_send.at[which, step - 1, 0], b_recv.at[which, step - 1, 0], dev=to)
                copy.start()
                second.append(copy)
            else:
                for y in range(n_y):
                    piece = m1.at[which, pl.ds((y * n_x + my_x) * half_boxes, half_boxes)]
                    to = my_y * n_x + lax.rem(my_x + step, n_x)
                    copy = remote(piece, piece, b_send.at[which, step - 1, y], b_recv.at[which, step - 1, y], dev=to)
                    copy.start()
                    second.append(copy)
    start_halo(range(max(FIRST_PIECES + 1, HALO_FIRST), HALO_LAST))
    for copy in d_copies:
        copy.wait_recv()
    other = grp + 1 - 2 * lax.rem(grp, 2)
    z_copies, c_copies = [], []
    for step in range(1, n_grp // 2):
        to = lax.rem(grp + 2 * step, n_grp)
        copy = remote(m2.at[grp], m2.at[grp], z_send.at[step - 1], z_recv.at[step - 1], grp=to)
        copy.start()
        z_copies.append(copy)
    copy = remote(m2.at[grp], m2.at[grp], c_send.at[0], c_recv.at[0], grp=other)
    copy.start()
    c_copies.append(copy)

    def couple(own, sources):
        spread = [jnp.broadcast_to(own[:, d : d + 1], (K, LANES)) for d in range(3)]
        total = jnp.zeros((R, K), jnp.float32)
        for first in range(0, len(sources), 4):
            highs, lows, parts = [], [], []
            for i in range(first, first + 4, 2):
                (v0, n0, odd0), (v1, n1, odd1) = sources[i], sources[i + 1]
                value = jnp.where(
                    low, jnp.concatenate([v0, swap(v0)], axis=0), jnp.concatenate([swap(v1), v1], axis=0)
                )
                n0 = jnp.where(odd0, swap(n0), n0)
                n1 = jnp.where(odd1, n1, swap(n1))
                place = jnp.where(low[:3], n0, n1) * 4.0
                d0, d1, d2 = (spread[d] - place[d : d + 1] for d in range(3))
                high, rest = split(lax.rsqrt(((1.0 + d0 * d0) + d1 * d1) + d2 * d2))
                highs.append(high)
                lows.append(rest)
                parts.append(value)
            value = jnp.concatenate(parts, axis=1)
            value_high, value_low = split(value)
            high, rest = jnp.concatenate(highs, axis=1), jnp.concatenate(lows, axis=1)
            both = dot(jnp.concatenate([value_high, value_low], axis=0), high, NT)
            total += both[:R] + both[R:] + dot(value_high, rest, NT)
        return total

    for copy in n_copies + second:
        copy.wait_recv()
    start_halo(range(HALO_LAST, PIECES))

    for step in range(1, n_grp // 2):
        z_copies[step - 1].wait_recv()
        block = m2.at[lax.rem(grp + n_grp - 2 * step, n_grp)]
        copy = remote(block, block, c_send.at[step], c_recv.at[step], grp=other)
        copy.start()
        c_copies.append(copy)

    def level_one(t, carry):
        sources = []
        for i in range(far1.shape[1]):
            s = lax.rem(far1[t, i], n_dev * boxes)
            home, box = lax.div(s, boxes), lax.rem(s, boxes)
            v = m1[lax.div(box, half_boxes), home * half_boxes + lax.rem(box, half_boxes)]
            both = near_nodes[home * (half_boxes // 2) + lax.div(box, 4)]
            n = jnp.where(lax.rem(lax.div(box, 2), 2) == 1, both[8:11], both[0:3])
            sources.append((v, n, lax.rem(box, 2) == 1))
        own = own_n[pl.ds(pl.multiple_of(t * K, K), K), :]
        acc[t, :, 0:HALF] = couple(own, sources)
        return carry

    lax.fori_loop(0, boxes, level_one, 0, unroll=2)

    for copy in c_copies:
        copy.wait_recv()

    def level_two(t, carry):
        target = box_parent[t]
        sources = []
        for i in range(far2.shape[0]):
            s = far2[i, target]
            v = m2[lax.div(s, n_dev), lax.rem(s, n_dev)]
            n = all_n2[lax.div(s, 2)][:3]
            sources.append((v, n, lax.rem(s, 2) == 1))
        own = own_n2[lax.rem(target, n_dev)]
        acc[t, :, HALF:LANES] = couple(own, sources)
        return carry

    lax.fori_loop(0, boxes, level_two, 0, unroll=2)

    for q in range(boxes // 2):
        rows = []
        for i in range(2):
            coarse = acc[2 * q + i]
            rows.append(jnp.where(low, swap(coarse), 0.0) if i == 0 else jnp.where(low, 0.0, coarse))
        moved = dot_split(jnp.concatenate(rows, axis=0), box_transfer[:, q * LANES : (q + 1) * LANES], NT)
        for i in range(2):
            g = acc[2 * q + i][:, :HALF] + moved[i * R : (i + 1) * R]
            g1[2 * q + i] = jnp.concatenate([g, g], axis=1)

    def descend(p, carry):
        top = g1[lax.rem(parent[2 * p], boxes)]
        bottom = g1[lax.rem(parent[2 * p + 1], boxes)]
        rows = jnp.concatenate([jnp.where(low, top, 0.0), jnp.where(low, 0.0, bottom)], axis=0)
        slab = transfer_v[:, pl.ds(pl.multiple_of(p * LANES, LANES), LANES)]
        high, rest = split(dot_split(rows, slab, NT))
        spread_g[p] = jnp.concatenate([high, rest, high], axis=1)
        return carry

    lax.fori_loop(0, leaves // 2, descend, 0, unroll=4)

    def evaluate(p, carry):
        left = spread_g[p]
        for i in range(2):
            at = pl.ds(pl.multiple_of((2 * p + i) * B, B), B)
            b_high, b_low = split(basis_v[:, at])
            far_out[:, at] = dot(left[i * R : (i + 1) * R], jnp.concatenate([b_high, b_high, b_low], axis=0), NN)
        return carry

    lax.fori_loop(0, leaves // 2, evaluate, 0, unroll=4)

    for copies in (n_copies, first, r_copies, d_copies, second, z_copies, c_copies):
        for copy in copies:
            copy.wait_send()
    for side in range(2):

        @pl.when(sends[side])
        def _():
            for copy in halo[side * per : (side + 1) * per]:
                copy.wait_send()

        @pl.when(sends[1 - side])
        def _():
            for copy in halo[side * per : (side + 1) * per]:
                copy.wait_recv()


def far_field(mesh_shape, count, parent, box_parent, far1, far2, points, rhs, basis, transfer, nodes, box_transfer, nodes2):
    n_grp, n_dev, n_x = mesh_shape
    n_y = n_dev // n_x
    boxes = box_parent.shape[0]
    leaves = count.shape[0]
    reach = REACH * B
    width = rhs.shape[1]
    vmem = pl.BlockSpec(memory_space=pltpu.VMEM)
    hbm = pl.BlockSpec(memory_space=pl.ANY)
    dma = pltpu.SemaphoreType.DMA
    small = (count, parent, box_parent, far1, far2)
    large = (nodes, box_transfer, nodes2, rhs, basis, transfer)
    return pl.pallas_call(
        functools.partial(far_kernel, mesh_shape),
        out_shape=(
            jax.ShapeDtypeStruct((2, R, reach), jnp.float32),
            jax.ShapeDtypeStruct((2, 3, reach), jnp.float32),
            jax.ShapeDtypeStruct((3, 1, leaves), jnp.int32),
            jax.ShapeDtypeStruct((R, width), jnp.float32),
        ),
        in_specs=[pl.BlockSpec(memory_space=pltpu.HBM)] * 13,
        out_specs=(hbm, hbm, hbm, vmem),
        scratch_shapes=[pltpu.SMEM(a.shape, jnp.int32) for a in small]
        + [pltpu.VMEM(a.shape, jnp.float32) for a in large]
        + [
            pltpu.VMEM((2, n_dev * (boxes // 2), 16, LANES), jnp.float32),
            pltpu.VMEM((n_dev * (boxes // 4), 16, LANES), jnp.float32),
            pltpu.VMEM((boxes, R, LANES), jnp.float32),
            pltpu.VMEM((boxes, R, LANES), jnp.float32),
            pltpu.VMEM((n_dev - 1, 16, LANES), jnp.float32),
            pltpu.VMEM((n_dev, 16, LANES), jnp.float32),
            pltpu.VMEM((n_grp, n_dev, 16, LANES), jnp.float32),
            pltpu.VMEM((boxes * K, 8), jnp.float32),
            pltpu.VMEM((n_dev, K, 8), jnp.float32),
            pltpu.VMEM((nodes2.shape[1] // LANES, 8, LANES), jnp.float32),
            pltpu.VMEM((leaves // 2, 2 * R, LANES), jnp.float32),
            pltpu.VMEM((leaves // 2, 2 * R, 3 * K), jnp.bfloat16),
            dma((11,)),
            dma((2, PIECES + 2)), dma((2, PIECES + 2)),
            dma((n_dev - 1,)), dma((n_dev - 1,)),
            dma((2, max(n_x, n_y) - 1)), dma((2, max(n_x, n_y) - 1)),
            dma((2, max(n_x, n_y) - 1, n_y)), dma((2, max(n_x, n_y) - 1, n_y)),
            dma((n_dev - 1,)), dma((n_dev - 1,)),
            dma((n_dev - 1,)), dma((n_dev - 1,)),
            dma((n_grp // 2 - 1,)), dma((n_grp // 2 - 1,)),
            dma((n_grp // 2,)), dma((n_grp // 2,)),
        ],
        compiler_params=pltpu.CompilerParams(collective_id=0, has_side_effects=True, vmem_limit_bytes=FAR_VMEM),
        cost_estimate=pl.CostEstimate(flops=10**9, bytes_accessed=10**7, transcendentals=10**6),
        name="far_field",
    )(count, parent, box_parent, far1, far2, points, rhs, basis, transfer, nodes, box_transfer, nodes2, count.reshape(1, 1, -1))


def local(
    mesh_shape,
    points,
    rhs,
    leaf_count,
    near_list,
    leaf_basis,
    leaf_transfer,
    leaf_parent,
    nodes1,
    box_transfer,
    box_parent,
    far1,
    nodes2,
    far2,
):
    halo_x, halo_p, halo_c, far = far_field(
        mesh_shape, leaf_count, leaf_parent, box_parent, far1, far2.T,
        points, rhs, leaf_basis, leaf_transfer, nodes1, box_transfer, nodes2,
    )
    return near_field(halo_c, leaf_count, near_list.T, halo_x, halo_p, rhs, points, far)


def solution(mesh):
    placed = (
        P(None, ("grp", "dev")),
        P(None, ("grp", "dev")),
        P(("grp", "dev")),
        P(("grp", "dev"), None),
        P(None, ("grp", "dev")),
        P(None, ("grp", "dev")),
        P(("grp", "dev")),
        P(None, ("grp", "dev")),
        P(None, ("grp", "dev")),
        P(("grp", "dev")),
        P(("grp", "dev"), None),
        P(),
        P(),
    )
    mesh_shape = (mesh.shape["grp"], mesh.shape["dev"], 4)
    return jax.shard_map(
        functools.partial(local, mesh_shape),
        mesh=mesh, in_specs=placed, out_specs=P(None, ("grp", "dev")), check_vma=False
    )
```

```python
import functools

import jax
import jax.numpy as jnp
from jax import lax
from jax.experimental import pallas as pl
from jax.experimental.pallas import tpu as pltpu
from jax.sharding import PartitionSpec as P

B = 256
K = 64
R = 32
NEAR = 8
REACH = 32
LANES = 128
TILE = 32
SLOTS = 2
NEAR_VMEM = 62 * 1024 * 1024


def near_kernel(
    leaves, halo_c_h, own_c_h, rel_h, halo_x_h, halo_p_h, own_x_h, own_p_h, far_h, out,
    halo_c, own_c, rel, halo_x, halo_p, own_x, own_p, far, sems,
    xs, pb, ab, sums, lists, cnt, bases, turns, accs,
):
    pairs = [
        (halo_c_h, halo_c), (own_c_h, own_c), (rel_h, rel), (own_x_h, own_x), (own_p_h, own_p),
        (halo_x_h, halo_x), (halo_p_h, halo_p), (far_h, far),
    ]
    loads = [pltpu.make_async_copy(src, dst, sems.at[i]) for i, (src, dst) in enumerate(pairs)]
    for copy in loads:
        copy.start()
    halo = halo_x.shape[2] // B
    total = leaves + 2 * halo
    first_leaf = (lax.axis_index("grp") * lax.axis_size("dev") + lax.axis_index("dev")) * leaves - halo
    for copy in loads[:3]:
        copy.wait()
    for i in range(halo):
        cnt[i] = halo_c[0, 0, leaves - halo + i]
        cnt[halo + leaves + i] = halo_c[2, 0, i]
    for i in range(leaves):
        cnt[halo + i] = own_c[i]
    lane = lax.broadcasted_iota(jnp.int32, (R, B), 1)

    def load_source(src_x, src_p, first, i):
        at = pl.ds(pl.multiple_of(i * B, B), B)
        to = pl.ds(pl.multiple_of((first + i) * B, B), B)
        x = jnp.where(lane < cnt[first + i], src_x[:, at], 0.0)
        high = x.astype(jnp.bfloat16)
        xs[0:R, to] = high
        xs[R : 2 * R, to] = (x - high.astype(jnp.float32)).astype(jnp.bfloat16)
        scaled = src_p[:, at] * 4.0
        pb[0:3, to] = scaled

    def load_halo(i, carry):
        load_source(halo_x.at[0], halo_p.at[0], 0, i)
        load_source(halo_x.at[1], halo_p.at[1], halo + leaves, i)
        return carry

    tail = pl.ds(total * B, 2 * LANES)
    xs[:, tail] = jnp.zeros((2 * R, 2 * LANES), jnp.bfloat16)
    pb[:, tail] = jnp.zeros((8, 2 * LANES), jnp.float32)

    def spread(target, slot, half):
        at = pl.ds(pl.multiple_of((halo + target) * B + half * LANES, LANES), LANES)
        rows = pl.ds(pl.multiple_of(half * LANES, LANES), LANES)
        for d in range(3):
            ab[slot, d, rows, :] = jnp.broadcast_to(pb[d : d + 1, at], (LANES, LANES)).T

    def load_own(i, carry):
        load_source(own_x, own_p, halo, i)
        return carry

    def list_blocks(target):
        start = bases[target]
        at = start
        for n in range(NEAR):
            src = rel[n, jnp.minimum(target, leaves - 1)] - first_leaf
            lists[at] = 2 * src
            lists[at + 1] = 2 * src + 1
            step = 1 + (cnt[src] > LANES).astype(jnp.int32)
            at = at + (jnp.where(target < OWN[2], 0, step) if n == 0 else step)
        lists[at] = 2 * total
        chunks = lax.div(at - start + 1, 2)
        at = start + 2 * chunks
        lists[at] = lists[at - 2]
        lists[at + 1] = lists[at - 1]
        turns[target] = chunks
        bases[target + 1] = start + 4 * lax.div(chunks + 1, 2)

    for copy in loads[3:5]:
        copy.wait()
    lax.fori_loop(0, leaves, load_own, 0, unroll=4)
    for copy in loads[5:]:
        copy.wait()
    lax.fori_loop(0, halo, load_halo, 0, unroll=2)
    for half in range(B // LANES):
        spread(0, 0, half)
    bases[0] = 0
    list_blocks(0)

    def push(start):
        for unit in range(2):
            parts = []
            for half in range(2):
                at = lists[start + 2 * unit + half]
                parts.append(xs[:, pl.ds(pl.multiple_of(at * LANES, LANES), LANES)])
            w = jnp.concatenate(parts, axis=1)
            pltpu.matmul_push_rhs(jnp.concatenate([w] * 4, axis=0), 0, unit, transpose=True)

    def pop(slot, target):
        for t in range(B // TILE):
            both = pltpu.matmul_pop(accs[0][slot][t]) + pltpu.matmul_pop(accs[1][slot][t])
            sums[target, t * TILE : (t + 1) * TILE, :] = both[:, :LANES]

    def couple_step(slot, tiles, target, start, split_rows):
        cols = []
        for unit in range(1 if split_rows else 2):
            halves = []
            for half in range(2):
                at = lists[start + 2 * unit + half]
                at = pl.ds(pl.multiple_of(at * LANES, LANES), LANES)
                halves.append([pb[d : d + 1, at] for d in range(3)])
            cols.append(halves)
        fresh = [True, True]
        waiting = [[], []]
        for t in range(tiles):
            own = [ab[slot, d, t * TILE : (t + 1) * TILE, :] for d in range(3)]
            for unit in [t % 2] if split_rows else range(2):
                highs, lows = [], []
                for half in range(2):
                    col = cols[0 if split_rows else unit][half]
                    d0, d1, d2 = (own[d] - col[d] for d in range(3))
                    k = lax.rsqrt(((1.0 + d0 * d0) + d1 * d1) + d2 * d2)
                    highs.append(k)
                    lows.append(k - k.astype(jnp.bfloat16).astype(jnp.float32))
                acc = accs[unit][slot][t]
                pltpu.matmul_acc_lhs(acc, jnp.concatenate(highs, axis=1), load_staged_rhs=0 if fresh[unit] else None)
                fresh[unit] = False
                for args in waiting[unit]:
                    pltpu.matmul_acc_lhs(*args)
                waiting[unit] = [(acc, jnp.concatenate(lows, axis=1))]
            if t == (1 if split_rows else 0):
                push(start + 4)
        for unit in range(2):
            for args in waiting[unit]:
                pltpu.matmul_acc_lhs(*args)

    def sweep(slot, tiles, target):
        start, count = bases[target], turns[target]

        def pair(i, carry):
            couple_step(slot, tiles, target, start + 4 * i, False)
            return carry

        list_blocks(target + 1)
        for i in range(2):
            couple_step(slot, tiles, target, start + 4 * i, False)
            spread(jnp.minimum(target + 1, leaves - 1), 1 - slot, i)
        lax.fori_loop(2, lax.div(count, 2), pair, 0)

        @pl.when(lax.rem(count, 2) == 1)
        def _():
            couple_step(slot, tiles, target, start + 2 * (count - 1), True)

    for slot in range(SLOTS):
        pop(slot, leaves)
    push(0)

    def group(g, carry):
        for slot in range(SLOTS):
            target = SLOTS * g + slot
            kind = lax.div(cnt[halo + target] + (TILE - 1), TILE) - 2
            lax.switch(kind, [functools.partial(sweep, slot, tiles, target) for tiles in range(2, B // TILE + 1)])
            pop(1 - slot, jnp.where(target == 0, leaves, target - 1))
        return carry

    lax.fori_loop(0, leaves // SLOTS, group, 0)
    for unit in range(2):
        pltpu.matmul_acc_lhs(accs[unit][0][0], jnp.zeros((TILE, 2 * LANES), jnp.bfloat16), load_staged_rhs=0)
    pop(1, leaves - 1)
    pop(0, leaves)

    def finish(target, carry):
        parts = []
        for half in range(B // LANES):
            flipped = sums[target, half * LANES : (half + 1) * LANES, :].T
            parts.append(flipped[0:R] + flipped[R : 2 * R])
        at = pl.ds(pl.multiple_of(target * B, B), B)
        value = jnp.concatenate(parts, axis=1) + far[:, at]
        out[:, at] = jnp.where(lane < cnt[halo + target], value, 0.0)
        return carry

    lax.fori_loop(0, leaves, finish, 0, unroll=4)


def near_body(leaves, *refs):
    tiles = B // TILE
    specs = tuple(
        tuple(tuple(pltpu.ACC(unit)((TILE, 256), jnp.float32) for _ in range(tiles)) for _ in range(SLOTS))
        for unit in range(2)
    )
    pl.run_scoped(lambda accs: near_kernel(leaves, *refs, accs), specs)


def near_field(halo_c, own_c, rel, halo_x, halo_p, own_x, own_p, far):
    leaves = own_x.shape[1] // B
    extent = leaves + 2 * (halo_x.shape[2] // B)
    wide = extent * B + 2 * LANES
    small = (halo_c, own_c, rel)
    large = (halo_x, halo_p, own_x, own_p, far)
    return pl.pallas_call(
        functools.partial(near_body, leaves),
        out_shape=jax.ShapeDtypeStruct((R, leaves * B), jnp.float32),
        in_specs=[pl.BlockSpec(memory_space=pl.ANY)] * 8,
        out_specs=pl.BlockSpec(memory_space=pltpu.VMEM),
        scratch_shapes=[pltpu.SMEM(a.shape, jnp.int32) for a in small]
        + [pltpu.VMEM(a.shape, jnp.float32) for a in large]
        + [
            pltpu.SemaphoreType.DMA((8,)),
            pltpu.VMEM((2 * R, wide), jnp.bfloat16),
            pltpu.VMEM((8, wide), jnp.float32),
            pltpu.VMEM((SLOTS, 3, B, LANES), jnp.float32),
            pltpu.VMEM((leaves + 1, B, LANES), jnp.float32),
            pltpu.SMEM((leaves * 16 + 40,), jnp.int32),
            pltpu.SMEM((extent,), jnp.int32),
            pltpu.SMEM((leaves + 2,), jnp.int32),
            pltpu.SMEM((leaves + 2,), jnp.int32),
        ],
        compiler_params=pltpu.CompilerParams(vmem_limit_bytes=NEAR_VMEM),
        cost_estimate=pl.CostEstimate(flops=10**9, bytes_accessed=10**7, transcendentals=10**7),
        name="near_field",
    )(halo_c, own_c, rel, halo_x, halo_p, own_x, own_p, far)


MESH = pl.DeviceIdType.MESH
HALF = 64
PIECES = 8
FIRST_PIECES = 1
HALO_FIRST = 0
HALO_LAST = 2
OWN = (8, 24, 40)
ALONG_X = (True, False)
FAR_VMEM = 62 * 1024 * 1024
NT = (((1,), (1,)), ((), ()))
NN = (((1,), (0,)), ((), ()))


def split(x):
    high = x.astype(jnp.bfloat16)
    return high, (x - high.astype(jnp.float32)).astype(jnp.bfloat16)


def dot(a, b, dims):
    return lax.dot_general(a, b, dims, preferred_element_type=jnp.float32)


def dot_split(a, b, dims):
    a_high, a_low = split(a)
    b_high, b_low = split(b)
    rows = a.shape[0]
    both = dot(jnp.concatenate([a_high, a_low], axis=0), b_high, dims)
    return both[:rows] + both[rows:] + dot(a_high, b_low, dims)


def swap(x):
    return pltpu.roll(x, HALF, 1)


def fold(x):
    lane = lax.broadcasted_iota(jnp.int32, (16, LANES), 1)
    return jnp.where(lane < HALF, x[:16], x[16:])


def far_kernel(
    shape,
    count_h, parent_h, box_parent_h, far1_h, far2_h,
    points, rhs, basis, transfer, nodes_h, box_transfer_h, nodes2_h, counts,
    halo_x, halo_p, halo_c, far_out,
    count, parent, box_parent, far1, far2, nodes, box_transfer, nodes2,
    x_v, basis_v, transfer_v, points_v, m1, near_nodes, acc, g1, part, partial, m2, own_n, own_n2, all_n2, expanded, spread_g,
    load_sems, halo_send, halo_recv, n_send, n_recv, a_send, a_recv, b_send, b_recv,
    r_send, r_recv, d_send, d_recv, z_send, z_recv, c_send, c_recv,
):
    n_grp, n_dev, n_x = shape
    grp, dev = lax.axis_index("grp"), lax.axis_index("dev")
    n_y = n_dev // n_x
    my_y, my_x = dev // n_x, lax.rem(dev, n_x)
    leaves = parent.shape[0]
    boxes = box_parent.shape[0]
    reach = halo_x.shape[2]
    half_boxes = boxes // 2
    low = lax.broadcasted_iota(jnp.int32, (R, LANES), 1) < HALF

    pairs = [
        (nodes_h, nodes), (count_h, count), (parent_h, parent), (rhs, x_v), (basis, basis_v), (transfer, transfer_v),
        (box_parent_h, box_parent), (box_transfer_h, box_transfer), (far1_h, far1), (far2_h, far2), (nodes2_h, nodes2),
        (points, points_v),
    ]
    loads = [pltpu.make_async_copy(src, dst, load_sems.at[i]) for i, (src, dst) in enumerate(pairs)]
    for copy in loads:
        copy.start()

    barrier = pltpu.get_barrier_semaphore()
    for step in range(1, n_dev):
        pl.semaphore_signal(barrier, inc=1, device_id={"dev": lax.rem(dev + step, n_dev)}, device_id_type=MESH)
    for to in [lax.rem(grp + 2 * step, n_grp) for step in range(1, n_grp // 2)] + [grp + 1 - 2 * lax.rem(grp, 2)]:
        pl.semaphore_signal(barrier, inc=1, device_id={"grp": to}, device_id_type=MESH)
    pl.semaphore_wait(barrier, n_dev - 1 + n_grp // 2)

    def remote(src, dst, send, recv, **place):
        return pltpu.make_async_remote_copy(
            src_ref=src, dst_ref=dst, send_sem=send, recv_sem=recv, device_id=place, device_id_type=MESH
        )

    width = x_v.shape[1]
    part_w = reach // PIECES
    halo = []
    for side in range(2):
        to = lax.rem(dev + (1 if side == 0 else n_dev - 1), n_dev)
        first = width - reach if side == 0 else 0
        for piece in range(PIECES):
            halo.append(
                remote(
                    rhs.at[:, pl.ds(first + piece * part_w, part_w)],
                    halo_x.at[side, :, pl.ds(piece * part_w, part_w)],
                    halo_send.at[side, piece],
                    halo_recv.at[side, piece],
                    dev=to,
                )
            )
        halo.append(
            remote(points.at[:, pl.ds(first, reach)], halo_p.at[side], halo_send.at[side, PIECES], halo_recv.at[side, PIECES], dev=to)
        )
        halo.append(
            remote(counts.at[0], halo_c.at[2 * side], halo_send.at[side, PIECES + 1], halo_recv.at[side, PIECES + 1], dev=to)
        )
    per = PIECES + 2
    sends = (dev < n_dev - 1, dev > 0)

    def start_halo(which):
        for side in range(2):

            @pl.when(sends[side])
            def _():
                for i in which:
                    halo[side * per + i].start()

    loads[0].wait()
    for q in range(half_boxes):
        near_nodes[dev * (half_boxes // 2) + q // 2, q % 2 * 8 : q % 2 * 8 + 3, :] = nodes[:, q * LANES : (q + 1) * LANES]
    own_nodes = near_nodes.at[pl.ds(dev * (half_boxes // 2), half_boxes // 2)]
    n_copies = []
    for step in range(1, n_dev):
        to = lax.rem(dev + step, n_dev)
        copy = remote(own_nodes, own_nodes, n_send.at[step - 1], n_recv.at[step - 1], dev=to)
        copy.start()
        n_copies.append(copy)
    start_halo([PIECES, PIECES + 1] + list(range(FIRST_PIECES)))

    acc[...] = jnp.zeros_like(acc)
    far_out[...] = jnp.zeros_like(far_out)
    for copy in loads[1:]:
        copy.wait()
    slot = lax.broadcasted_iota(jnp.int32, (R, B), 1)

    def expand(p, carry):
        for i in range(2):
            c = 2 * p + i
            at = pl.ds(pl.multiple_of(c * B, B), B)
            x = jnp.where(slot < count[c], x_v[:, at], 0.0)
            x_high, x_low = split(x)
            b_high, b_low = split(basis_v[:, at])
            both = dot(jnp.concatenate([x_high, x_low], axis=0), jnp.concatenate([b_high, b_low], axis=0), NT)
            top, bottom = both[:R], both[R:]
            expanded[p, i * R : (i + 1) * R, :] = top + bottom + swap(top)
        return carry

    lax.fori_loop(0, leaves // 2, expand, 0, unroll=4)

    def lift(p, carry):
        slab = transfer_v[:, pl.ds(pl.multiple_of(p * LANES, LANES), LANES)]
        out = dot_split(expanded[p][:, :HALF], slab, NN)
        value = jnp.where(low, out[:R], out[R:])
        owner = jnp.where(low, parent[2 * p], parent[2 * p + 1]) - (grp * n_dev + dev) * boxes
        for b in range(boxes):
            acc[b] += jnp.where(owner == b, value, 0.0)
        return carry

    lax.fori_loop(0, leaves // 2, lift, 0, unroll=4)

    for b in range(boxes):
        full = acc[b] + swap(acc[b])
        acc[b] = full
        m1[b // half_boxes, dev * half_boxes + b % half_boxes] = fold(full)
    first, second = [], []

    def along(which, block, to, sem, copies):
        copy = remote(block, block, a_send.at[which, sem], a_recv.at[which, sem], dev=to)
        copy.start()
        copies.append(copy)

    mine = [m1.at[i, pl.ds(dev * half_boxes, half_boxes)] for i in range(2)]
    for which, along_x in enumerate(ALONG_X):
        for step in range(1, n_x if along_x else n_y):
            to = my_y * n_x + lax.rem(my_x + step, n_x) if along_x else lax.rem(my_y + step, n_y) * n_x + my_x
            along(which, mine[which], to, step - 1, first)

    sums = [jnp.zeros((16, LANES), jnp.float32) for _ in range(n_dev)]
    for q in range(boxes // 2):
        pair = jnp.concatenate([acc[2 * q], acc[2 * q + 1]], axis=0)[:, :HALF]
        out = dot_split(pair, box_transfer[:, q * LANES : (q + 1) * LANES], NN)
        for i in range(2):
            half = jnp.where(low == (i == 0), out[i * R : (i + 1) * R], 0.0)
            folded = fold(half + swap(half))
            owner = box_parent[2 * q + i] - grp * n_dev
            for p in range(n_dev):
                sums[p] += jnp.where(owner == p, folded, 0.0)
    for p in range(n_dev):
        partial[p] = sums[p]
    r_copies = []
    for step in range(1, n_dev):
        to = lax.rem(dev + step, n_dev)
        copy = remote(partial.at[to], part.at[step - 1], r_send.at[step - 1], r_recv.at[step - 1], dev=to)
        copy.start()
        r_copies.append(copy)
    start_halo(range(FIRST_PIECES, FIRST_PIECES + 1))

    for q in range(boxes // 2):
        own_n[q * LANES : (q + 1) * LANES, :] = (
            jnp.concatenate([nodes[:, q * LANES : (q + 1) * LANES], jnp.zeros((5, LANES), jnp.float32)], axis=0) * 4.0
        ).T
    for q in range(n_dev // 2):
        at = pl.ds(pl.multiple_of((grp * n_dev // 2 + q) * LANES, LANES), LANES)
        flipped = (jnp.concatenate([nodes2[:, at], jnp.zeros((5, LANES), jnp.float32)], axis=0) * 4.0).T
        own_n2[2 * q] = flipped[:K]
        own_n2[2 * q + 1] = flipped[K:]

    def spread_nodes(q, carry):
        all_n2[q, 0:3, :] = nodes2[:, pl.ds(pl.multiple_of(q * LANES, LANES), LANES)]
        return carry

    lax.fori_loop(0, nodes2.shape[1] // LANES, spread_nodes, 0, unroll=8)

    def own_block_field(c, carry):
        at = pl.ds(pl.multiple_of(c * B, B), B)
        x_high, x_low = split(jnp.where(slot < count[c], x_v[:, at], 0.0))
        both_x = jnp.concatenate([x_high, x_low], axis=0)
        place = points_v[:, at] * 4.0
        highs, lows = [], []
        for half in range(B // LANES):
            dist = jnp.ones((LANES, B), jnp.float32)
            for d in range(3):
                row = place[d : d + 1, half * LANES : (half + 1) * LANES]
                spread = jnp.broadcast_to(row, (LANES, LANES)).T
                diff = jnp.concatenate([spread, spread], axis=1) - place[d : d + 1]
                dist = dist + diff * diff
            high, rest = split(lax.rsqrt(dist))
            highs.append(high)
            lows.append(rest)
        value = dot(both_x, jnp.concatenate(highs, axis=0), NN) + dot(both_x, jnp.concatenate(lows, axis=0), NN)
        far_out[:, at] += value[:R] + value[R:]
        return carry

    lax.fori_loop(0, OWN[0], own_block_field, 0, unroll=4)
    total = partial[dev]
    for step in range(1, n_dev):
        r_copies[step - 1].wait_recv()
        total += part[step - 1]
    m2[grp, dev] = total
    d_copies = []
    for step in range(1, n_dev):
        to = lax.rem(dev + step, n_dev)
        copy = remote(m2.at[grp, dev], m2.at[grp, dev], d_send.at[step - 1], d_recv.at[step - 1], dev=to)
        copy.start()
        d_copies.append(copy)
    for copy in first:
        copy.wait_recv()
    if HALO_FIRST:
        start_halo(range(FIRST_PIECES + 1, HALO_FIRST))
    for which, along_x in enumerate(ALONG_X):
        for step in range(1, n_y if along_x else n_x):
            if along_x:
                row = m1.at[which, pl.ds(my_y * n_x * half_boxes, n_x * half_boxes)]
                to = lax.rem(my_y + step, n_y) * n_x + my_x
                copy = remote(row, row, b_send.at[which, step - 1, 0], b_recv.at[which, step - 1, 0], dev=to)
                copy.start()
                second.append(copy)
            else:
                for y in range(n_y):
                    piece = m1.at[which, pl.ds((y * n_x + my_x) * half_boxes, half_boxes)]
                    to = my_y * n_x + lax.rem(my_x + step, n_x)
                    copy = remote(piece, piece, b_send.at[which, step - 1, y], b_recv.at[which, step - 1, y], dev=to)
                    copy.start()
                    second.append(copy)
    start_halo(range(max(FIRST_PIECES + 1, HALO_FIRST), HALO_LAST))
    for copy in d_copies:
        copy.wait_recv()
    other = grp + 1 - 2 * lax.rem(grp, 2)
    z_copies, c_copies = [], []
    for step in range(1, n_grp // 2):
        to = lax.rem(grp + 2 * step, n_grp)
        copy = remote(m2.at[grp], m2.at[grp], z_send.at[step - 1], z_recv.at[step - 1], grp=to)
        copy.start()
        z_copies.append(copy)
    copy = remote(m2.at[grp], m2.at[grp], c_send.at[0], c_recv.at[0], grp=other)
    copy.start()
    c_copies.append(copy)

    def couple(own, sources):
        spread = [jnp.broadcast_to(own[:, d : d + 1], (K, LANES)) for d in range(3)]
        total = jnp.zeros((R, K), jnp.float32)
        for first in range(0, len(sources), 4):
            highs, lows, parts = [], [], []
            for i in range(first, first + 4, 2):
                (v0, n0, odd0), (v1, n1, odd1) = sources[i], sources[i + 1]
                value = jnp.where(
                    low, jnp.concatenate([v0, swap(v0)], axis=0), jnp.concatenate([swap(v1), v1], axis=0)
                )
                n0 = jnp.where(odd0, swap(n0), n0)
                n1 = jnp.where(odd1, n1, swap(n1))
                place = jnp.where(low[:3], n0, n1) * 4.0
                d0, d1, d2 = (spread[d] - place[d : d + 1] for d in range(3))
                high, rest = split(lax.rsqrt(((1.0 + d0 * d0) + d1 * d1) + d2 * d2))
                highs.append(high)
                lows.append(rest)
                parts.append(value)
            value = jnp.concatenate(parts, axis=1)
            value_high, value_low = split(value)
            high, rest = jnp.concatenate(highs, axis=1), jnp.concatenate(lows, axis=1)
            both = dot(jnp.concatenate([value_high, value_low], axis=0), high, NT)
            total += both[:R] + both[R:] + dot(value_high, rest, NT)
        return total

    lax.fori_loop(OWN[0], OWN[1], own_block_field, 0, unroll=4)
    for copy in n_copies + second:
        copy.wait_recv()
    start_halo(range(HALO_LAST, PIECES))

    for step in range(1, n_grp // 2):
        z_copies[step - 1].wait_recv()
        block = m2.at[lax.rem(grp + n_grp - 2 * step, n_grp)]
        copy = remote(block, block, c_send.at[step], c_recv.at[step], grp=other)
        copy.start()
        c_copies.append(copy)

    def level_one(t, carry):
        sources = []
        for i in range(far1.shape[1]):
            s = lax.rem(far1[t, i], n_dev * boxes)
            home, box = lax.div(s, boxes), lax.rem(s, boxes)
            v = m1[lax.div(box, half_boxes), home * half_boxes + lax.rem(box, half_boxes)]
            both = near_nodes[home * (half_boxes // 2) + lax.div(box, 4)]
            n = jnp.where(lax.rem(lax.div(box, 2), 2) == 1, both[8:11], both[0:3])
            sources.append((v, n, lax.rem(box, 2) == 1))
        own = own_n[pl.ds(pl.multiple_of(t * K, K), K), :]
        acc[t, :, 0:HALF] = couple(own, sources)
        return carry

    lax.fori_loop(0, boxes, level_one, 0, unroll=2)

    for copy in c_copies:
        copy.wait_recv()

    def level_two(t, carry):
        target = box_parent[t]
        sources = []
        for i in range(far2.shape[0]):
            s = far2[i, target]
            v = m2[lax.div(s, n_dev), lax.rem(s, n_dev)]
            n = all_n2[lax.div(s, 2)][:3]
            sources.append((v, n, lax.rem(s, 2) == 1))
        own = own_n2[lax.rem(target, n_dev)]
        acc[t, :, HALF:LANES] = couple(own, sources)
        return carry

    lax.fori_loop(0, boxes, level_two, 0, unroll=2)

    for q in range(boxes // 2):
        rows = []
        for i in range(2):
            coarse = acc[2 * q + i]
            rows.append(jnp.where(low, swap(coarse), 0.0) if i == 0 else jnp.where(low, 0.0, coarse))
        moved = dot_split(jnp.concatenate(rows, axis=0), box_transfer[:, q * LANES : (q + 1) * LANES], NT)
        for i in range(2):
            g = acc[2 * q + i][:, :HALF] + moved[i * R : (i + 1) * R]
            g1[2 * q + i] = jnp.concatenate([g, g], axis=1)

    def descend(p, carry):
        top = g1[lax.rem(parent[2 * p], boxes)]
        bottom = g1[lax.rem(parent[2 * p + 1], boxes)]
        rows = jnp.concatenate([jnp.where(low, top, 0.0), jnp.where(low, 0.0, bottom)], axis=0)
        slab = transfer_v[:, pl.ds(pl.multiple_of(p * LANES, LANES), LANES)]
        high, rest = split(dot_split(rows, slab, NT))
        spread_g[p] = jnp.concatenate([high, rest, high], axis=1)
        return carry

    lax.fori_loop(0, leaves // 2, descend, 0, unroll=4)

    def evaluate(p, carry):
        left = spread_g[p]
        for i in range(2):
            at = pl.ds(pl.multiple_of((2 * p + i) * B, B), B)
            b_high, b_low = split(basis_v[:, at])
            value = dot(left[i * R : (i + 1) * R], jnp.concatenate([b_high, b_high, b_low], axis=0), NN)
            far_out[:, at] += value
        return carry

    lax.fori_loop(0, leaves // 2, evaluate, 0, unroll=4)
    lax.fori_loop(OWN[1], OWN[2], own_block_field, 0, unroll=4)

    for copies in (n_copies, first, r_copies, d_copies, second, z_copies, c_copies):
        for copy in copies:
            copy.wait_send()
    for side in range(2):

        @pl.when(sends[side])
        def _():
            for copy in halo[side * per : (side + 1) * per]:
                copy.wait_send()

        @pl.when(sends[1 - side])
        def _():
            for copy in halo[side * per : (side + 1) * per]:
                copy.wait_recv()


def far_field(mesh_shape, count, parent, box_parent, far1, far2, points, rhs, basis, transfer, nodes, box_transfer, nodes2):
    n_grp, n_dev, n_x = mesh_shape
    n_y = n_dev // n_x
    boxes = box_parent.shape[0]
    leaves = count.shape[0]
    reach = REACH * B
    width = rhs.shape[1]
    vmem = pl.BlockSpec(memory_space=pltpu.VMEM)
    hbm = pl.BlockSpec(memory_space=pl.ANY)
    dma = pltpu.SemaphoreType.DMA
    small = (count, parent, box_parent, far1, far2)
    large = (nodes, box_transfer, nodes2, rhs, basis, transfer, points)
    return pl.pallas_call(
        functools.partial(far_kernel, mesh_shape),
        out_shape=(
            jax.ShapeDtypeStruct((2, R, reach), jnp.float32),
            jax.ShapeDtypeStruct((2, 3, reach), jnp.float32),
            jax.ShapeDtypeStruct((3, 1, leaves), jnp.int32),
            jax.ShapeDtypeStruct((R, width), jnp.float32),
        ),
        in_specs=[pl.BlockSpec(memory_space=pltpu.HBM)] * 13,
        out_specs=(hbm, hbm, hbm, vmem),
        scratch_shapes=[pltpu.SMEM(a.shape, jnp.int32) for a in small]
        + [pltpu.VMEM(a.shape, jnp.float32) for a in large]
        + [
            pltpu.VMEM((2, n_dev * (boxes // 2), 16, LANES), jnp.float32),
            pltpu.VMEM((n_dev * (boxes // 4), 16, LANES), jnp.float32),
            pltpu.VMEM((boxes, R, LANES), jnp.float32),
            pltpu.VMEM((boxes, R, LANES), jnp.float32),
            pltpu.VMEM((n_dev - 1, 16, LANES), jnp.float32),
            pltpu.VMEM((n_dev, 16, LANES), jnp.float32),
            pltpu.VMEM((n_grp, n_dev, 16, LANES), jnp.float32),
            pltpu.VMEM((boxes * K, 8), jnp.float32),
            pltpu.VMEM((n_dev, K, 8), jnp.float32),
            pltpu.VMEM((nodes2.shape[1] // LANES, 8, LANES), jnp.float32),
            pltpu.VMEM((leaves // 2, 2 * R, LANES), jnp.float32),
            pltpu.VMEM((leaves // 2, 2 * R, 3 * K), jnp.bfloat16),
            dma((12,)),
            dma((2, PIECES + 2)), dma((2, PIECES + 2)),
            dma((n_dev - 1,)), dma((n_dev - 1,)),
            dma((2, max(n_x, n_y) - 1)), dma((2, max(n_x, n_y) - 1)),
            dma((2, max(n_x, n_y) - 1, n_y)), dma((2, max(n_x, n_y) - 1, n_y)),
            dma((n_dev - 1,)), dma((n_dev - 1,)),
            dma((n_dev - 1,)), dma((n_dev - 1,)),
            dma((n_grp // 2 - 1,)), dma((n_grp // 2 - 1,)),
            dma((n_grp // 2,)), dma((n_grp // 2,)),
        ],
        compiler_params=pltpu.CompilerParams(collective_id=0, has_side_effects=True, vmem_limit_bytes=FAR_VMEM),
        cost_estimate=pl.CostEstimate(flops=10**9, bytes_accessed=10**7, transcendentals=10**6),
        name="far_field",
    )(count, parent, box_parent, far1, far2, points, rhs, basis, transfer, nodes, box_transfer, nodes2, count.reshape(1, 1, -1))


def local(
    mesh_shape,
    points,
    rhs,
    leaf_count,
    near_list,
    leaf_basis,
    leaf_transfer,
    leaf_parent,
    nodes1,
    box_transfer,
    box_parent,
    far1,
    nodes2,
    far2,
):
    halo_x, halo_p, halo_c, far = far_field(
        mesh_shape, leaf_count, leaf_parent, box_parent, far1, far2.T,
        points, rhs, leaf_basis, leaf_transfer, nodes1, box_transfer, nodes2,
    )
    return near_field(halo_c, leaf_count, near_list.T, halo_x, halo_p, rhs, points, far)


def solution(mesh):
    placed = (
        P(None, ("grp", "dev")),
        P(None, ("grp", "dev")),
        P(("grp", "dev")),
        P(("grp", "dev"), None),
        P(None, ("grp", "dev")),
        P(None, ("grp", "dev")),
        P(("grp", "dev")),
        P(None, ("grp", "dev")),
        P(None, ("grp", "dev")),
        P(("grp", "dev")),
        P(("grp", "dev"), None),
        P(),
        P(),
    )
    mesh_shape = (mesh.shape["grp"], mesh.shape["dev"], 4)
    return jax.shard_map(
        functools.partial(local, mesh_shape),
        mesh=mesh, in_specs=placed, out_specs=P(None, ("grp", "dev")), check_vma=False
    )
```
